32 devices in a mesh: tp: 32 (over z, y, x, core).
Axes of the slice: x: 2, y: 2, z: 4, core: 2. Of those that a mesh axis runs over, the one named last changes fastest.
Arguments:
- x_norm: bfloat16 [4096, 2048], P(None, 'tp')
- hid_act: bfloat16 [4096, 5120], P(None, 'tp')
- dy_in: bfloat16 [2, 4096, 5120], replicated
- dy_out: bfloat16 [4096, 2048], replicated
- w_in: float32 [2, 2048, 5120], P(None, 'tp')
- w_out: float32 [5120, 2048], P('tp')
- row_in: float32 [2, 2048], P(None, 'tp')
- col_in: float32 [2, 5120], replicated
- row_out: float32 [5120], P('tp')
- col_out: float32 [2048], replicated
- beta_two: float32 [], replicated
- rel_step: float32 [], replicated
- clip_rms: float32 [], replicated
- clip_norm: float32 [], replicated
Outputs:
- output 1: float32 [2, 2048, 5120], P(None, 'tp')
- output 2: float32 [2, 2048], P(None, 'tp')
- output 3: float32 [2, 5120], replicated
- output 4: float32 [5120, 2048], P('tp')
- output 5: float32 [5120], P('tp')
- output 6: float32 [2048], replicated
All inputs are finite; a program needn't handle non-finite values.
Results may differ from the reference program's by a relative error of at most 0.001.
Values are sent between devices in bfloat16 or wider.
A program may use at most 1 GiB of HBM per device.

```python
import jax
import jax.numpy as jnp
from jax import lax

D = 2048
FF = 5120
TOK_DEV = 128
GROUP = 32
TOKENS = TOK_DEV * GROUP
EPS_ONE = 1e-30
EPS_TWO = 1e-3


def setup_inputs(seed: int = 0) -> dict:
    key_list = jax.random.split(jax.random.key(seed), 14)
    x_norm = jax.random.normal(key_list[0], (TOKENS, D), jnp.float32).astype(jnp.bfloat16)
    hid_act = jax.random.normal(key_list[1], (TOKENS, FF), jnp.float32).astype(jnp.bfloat16)
    dy_in = jax.random.normal(key_list[2], (2, TOKENS, FF), jnp.float32).astype(jnp.bfloat16)
    dy_out = jax.random.normal(key_list[3], (TOKENS, D), jnp.float32).astype(jnp.bfloat16)
    w_in = jax.random.normal(key_list[4], (2, D, FF), jnp.float32) * (D ** -0.5)
    w_out = jax.random.normal(key_list[5], (FF, D), jnp.float32) * (FF ** -0.5)
    stat_level = 0.2 * TOKENS
    row_in = stat_level * jax.random.uniform(key_list[6], (2, D), jnp.float32, minval=0.3, maxval=1.7)
    col_in = stat_level * jax.random.uniform(key_list[7], (2, FF), jnp.float32, minval=0.3, maxval=1.7)
    row_out = stat_level * jax.random.uniform(key_list[8], (FF,), jnp.float32, minval=0.3, maxval=1.7)
    col_out = stat_level * jax.random.uniform(key_list[9], (D,), jnp.float32, minval=0.3, maxval=1.7)
    beta_two = jax.random.uniform(key_list[10], (), jnp.float32, minval=0.5, maxval=0.9)
    rel_step = jax.random.uniform(key_list[11], (), jnp.float32, minval=0.2, maxval=0.8)
    clip_rms = jax.random.uniform(key_list[12], (), jnp.float32, minval=0.2, maxval=0.4)
    clip_frac = jax.random.uniform(key_list[13], (), jnp.float32, minval=0.35, maxval=0.6)
    clip_norm = clip_frac * (3.0 * TOKENS * D * FF) ** 0.5
    return {"x_norm": x_norm, "hid_act": hid_act, "dy_in": dy_in, "dy_out": dy_out,
            "w_in": w_in, "w_out": w_out, "row_in": row_in, "col_in": col_in,
            "row_out": row_out, "col_out": col_out, "beta_two": beta_two,
            "rel_step": rel_step, "clip_rms": clip_rms, "clip_norm": clip_norm}


def adafactor_update(weight, gradient, row_stat, col_stat, beta_two, rel_step, clip_rms, grad_scale):
    scaled = grad_scale * gradient
    sq_grad = scaled * scaled + EPS_ONE
    mix_new = 1.0 - beta_two
    row_new = beta_two * row_stat + mix_new * jnp.mean(sq_grad, axis=-1)
    col_new = beta_two * col_stat + mix_new * jnp.mean(sq_grad, axis=-2)
    row_level = jnp.mean(row_new, axis=-1, keepdims=True)
    second = (row_new / row_level)[..., :, None] * col_new[..., None, :]
    update = scaled / jnp.sqrt(second)
    upd_rms = jnp.sqrt(jnp.mean(update * update, axis=(-2, -1), keepdims=True))
    clipped = update / jnp.maximum(1.0, upd_rms / clip_rms)
    w_rms = jnp.sqrt(jnp.mean(weight * weight, axis=(-2, -1), keepdims=True))
    step_size = rel_step * jnp.maximum(EPS_TWO, w_rms)
    return weight - step_size * clipped, row_new, col_new


def reference(x_norm, hid_act, dy_in, dy_out, w_in, w_out, row_in, col_in, row_out, col_out, beta_two, rel_step, clip_rms, clip_norm):
    def input_grad(dy_one):
        return jnp.dot(x_norm.T, dy_one, preferred_element_type=jnp.float32)
    grad_in = lax.map(input_grad, dy_in)
    grad_out = jnp.dot(hid_act.T, dy_out, preferred_element_type=jnp.float32)
    norm_sq = jnp.sum(grad_in * grad_in) + jnp.sum(grad_out * grad_out)
    grad_scale = jnp.minimum(1.0, clip_norm / jnp.sqrt(norm_sq))
    new_in = adafactor_update(w_in, grad_in, row_in, col_in, beta_two, rel_step, clip_rms, grad_scale)
    new_out = adafactor_update(w_out, grad_out, row_out, col_out, beta_two, rel_step, clip_rms, grad_scale)
    return (new_in[0], new_in[1], new_in[2], new_out[0], new_out[1], new_out[2])
```

```python
import jax
import jax.numpy as jnp
from jax import lax
from jax.experimental import pallas as pl
from jax.experimental.pallas import tpu as pltpu
from jax.sharding import PartitionSpec as P

EPS_ONE = 1e-30
EPS_TWO = 1e-3
LANES = 128


def peer_barrier(me, n):
    barrier = pltpu.get_barrier_semaphore()
    for d in range(1, n):
        pl.semaphore_signal(barrier, inc=1, device_id=(lax.rem(me + d, n),), device_id_type=pl.DeviceIdType.MESH)
    pl.semaphore_wait(barrier, n - 1)


def reduce_kernel(n, x_ref, out_ref, landed, owned, sems):
    me = lax.axis_index('tp')
    peer_barrier(me, n)

    def send(src, dst, phase):
        for d in range(1, n):
            peer = lax.rem(me + d, n)
            pltpu.make_async_remote_copy(src_ref=src(peer), dst_ref=dst, send_sem=sems.at[phase, 0], recv_sem=sems.at[phase, 1],
                                         device_id=(peer,), device_id_type=pl.DeviceIdType.MESH).start()

    def wait(side, phase):
        pltpu.make_async_copy(x_ref.at[pl.ds(0, n - 1)], landed.at[pl.ds(0, n - 1)], sems.at[phase, side]).wait()

    send(lambda peer: x_ref.at[peer], landed.at[me], 0)
    landed[me] = x_ref[me]
    wait(1, 0)
    total = jnp.sum(landed[...], axis=0)
    owned[...] = total
    out_ref[me] = total
    send(lambda peer: owned, out_ref.at[me], 1)
    wait(1, 1)
    wait(0, 0)
    wait(0, 1)


def all_sum(x, n):
    return pl.pallas_call(
        lambda *refs: reduce_kernel(n, *refs),
        out_shape=jax.ShapeDtypeStruct(x.shape, x.dtype),
        in_specs=[pl.BlockSpec(memory_space=pltpu.VMEM)],
        out_specs=pl.BlockSpec(memory_space=pltpu.VMEM),
        scratch_shapes=[pltpu.VMEM(x.shape, x.dtype), pltpu.VMEM(x.shape[1:], x.dtype), pltpu.SemaphoreType.DMA((2, 2))],
        compiler_params=pltpu.CompilerParams(collective_id=0, has_side_effects=True),
        name='all_sum',
    )(x)


def gather_kernel(n, x_ref, out_ref, landed, sems):
    me = lax.axis_index('tp')
    peer_barrier(me, n)
    for d in range(1, n):
        peer = lax.rem(me + d, n)
        pltpu.make_async_remote_copy(src_ref=x_ref, dst_ref=landed.at[me], send_sem=sems.at[0], recv_sem=sems.at[1],
                                     device_id=(peer,), device_id_type=pl.DeviceIdType.MESH).start()
    landed[me] = x_ref[...]
    pltpu.make_async_copy(landed.at[pl.ds(0, n - 1)], landed.at[pl.ds(0, n - 1)], sems.at[1]).wait()
    out_ref[...] = jnp.sum(landed[...], axis=0)
    pltpu.make_async_copy(landed.at[pl.ds(0, n - 1)], landed.at[pl.ds(0, n - 1)], sems.at[0]).wait()


def small_sum(x, n):
    return pl.pallas_call(
        lambda *refs: gather_kernel(n, *refs),
        out_shape=jax.ShapeDtypeStruct(x.shape, x.dtype),
        in_specs=[pl.BlockSpec(memory_space=pltpu.VMEM)],
        out_specs=pl.BlockSpec(memory_space=pltpu.VMEM),
        scratch_shapes=[pltpu.VMEM((n,) + x.shape, x.dtype), pltpu.SemaphoreType.DMA((2,))],
        compiler_params=pltpu.CompilerParams(collective_id=1, has_side_effects=True),
        name='small_sum',
    )(x)


def solution(mesh):
    shards = mesh.shape['tp']

    def local_step(x_norm, hid_act, dy_in, dy_out, w_in, w_out, row_in, col_in, row_out, col_out, beta_two, rel_step, clip_rms, clip_norm):
        grad_in = jnp.einsum('ti,ktj->kij', x_norm, dy_in, preferred_element_type=jnp.float32)
        grad_out = jnp.einsum('ti,tj->ij', hid_act, dy_out, preferred_element_type=jnp.float32)
        kinds, cols_in = grad_in.shape[0], grad_in.shape[2]
        cols_out = grad_out.shape[1]
        col_local = jnp.concatenate([jnp.sum(grad_in * grad_in, axis=1).reshape(-1), jnp.sum(grad_out * grad_out, axis=0)])
        scalars = jnp.concatenate([jnp.sum(row_in, axis=1), jnp.sum(row_out)[None],
                                   jnp.sum(w_in * w_in, axis=(1, 2)), jnp.sum(w_out * w_out)[None]])
        scalars = jnp.broadcast_to(jnp.pad(scalars, (0, LANES - 6)), (shards, 1, LANES))
        block = jnp.concatenate([col_local.reshape(shards, -1, LANES), scalars], axis=1)
        total = all_sum(block, shards)
        col_all = total[:, :-1].reshape(-1)
        sums = total[0, -1]
        grad_scale = jnp.minimum(1.0, clip_norm / jnp.sqrt(jnp.sum(col_all)))
        sq_scale = grad_scale * grad_scale
        mix_new = 1.0 - beta_two

        def stats(grad, row_stat, col_stat, col_sq, row_sum):
            rows_total, col_count = grad.shape[0] * shards, grad.shape[1]
            row_new = beta_two * row_stat + mix_new * (sq_scale * jnp.mean(grad * grad, axis=-1) + EPS_ONE)
            col_new = beta_two * col_stat + mix_new * (sq_scale * col_sq / rows_total + EPS_ONE)
            level = beta_two * row_sum / rows_total + mix_new * (sq_scale * jnp.sum(col_sq) / (rows_total * col_count) + EPS_ONE)
            update = (grad_scale * grad) * lax.rsqrt(row_new / level)[:, None] * lax.rsqrt(col_new)[None, :]
            return row_new, col_new, update, jnp.sum(update * update)

        parts = [stats(grad_in[k], row_in[k], col_in[k], col_all[k * cols_in:(k + 1) * cols_in], sums[k]) for k in range(kinds)]
        parts.append(stats(grad_out, row_out, col_out, col_all[kinds * cols_in:], sums[kinds]))
        upd = jnp.stack([p[3] for p in parts])
        upd = small_sum(jnp.broadcast_to(jnp.pad(upd, (0, LANES - 3)), (8, LANES)), shards)[0, :3]

        def apply(weight, update, k):
            count = weight.size * shards
            clip = jnp.maximum(1.0, jnp.sqrt(upd[k] / count) / clip_rms)
            step = rel_step * jnp.maximum(EPS_TWO, jnp.sqrt(sums[3 + k] / count))
            return weight - step * (update / clip)

        new_in = jnp.stack([apply(w_in[k], parts[k][2], k) for k in range(kinds)])
        new_out = apply(w_out, parts[2][2], 2)
        return (new_in, jnp.stack([parts[0][0], parts[1][0]]), jnp.stack([parts[0][1], parts[1][1]]),
                new_out, parts[2][0], parts[2][1])

    in_specs = (P(None, 'tp'), P(None, 'tp'), P(), P(), P(None, 'tp', None), P('tp', None),
                P(None, 'tp'), P(), P('tp'), P(), P(), P(), P(), P())
    out_specs = (P(None, 'tp', None), P(None, 'tp'), P(), P('tp', None), P('tp'), P())
    return jax.shard_map(local_step, mesh=mesh, in_specs=in_specs, out_specs=out_specs, check_vma=False)
```

```python
import jax
import jax.numpy as jnp
from jax import lax
from jax.experimental import pallas as pl
from jax.experimental.pallas import tpu as pltpu
from jax.sharding import PartitionSpec as P

EPS_ONE = 1e-30
EPS_TWO = 1e-3
LANES = 128
STRIPE = 512
BLOCKS = STRIPE // LANES
EARLY = 8
LATE = 4
F32 = jnp.float32
MESH = pl.DeviceIdType.MESH


def grads_kernel(n, x_hbm, h_hbm, dyi_hbm, dyo_hbm, wi_hbm, wo_hbm, ri_hbm, ci_hbm, ro_hbm, co_hbm,
                 beta_hbm, step_hbm, rms_hbm, norm_hbm,
                 gi, go, wi, wo, ri_new, ci_new, ro_new, co_new, coef,
                 xs, hs, dy, si, so, csend, rs_land, ag_send, ag_land, late_land, csum, colf, ai, ao,
                 fsend, f_land, ri, ci, ro, co, beta, step, rms, norm,
                 dy_sem, x_sem, w_sem, small_sem, xs_sem, g_sem, rs_sem, ag_sem, late_sem, f_sem):
    me = lax.axis_index('tp')
    core = lax.rem(me, 2)
    chip = me // 2
    x, y, z = lax.rem(chip, 2), lax.rem(chip // 2, 2), chip // 4
    partner = me + 1 - 2 * core
    peers = []
    for dz in (2, 1, 3, 0):
        for dy_ in (1, 0):
            for dx in (1, 0):
                for dc in (0, 1):
                    if dz or dy_ or dx or dc:
                        peers.append(((lax.rem(z + dz, n // 8) * 2 + lax.rem(y + dy_, 2)) * 2 + lax.rem(x + dx, 2)) * 2
                                     + lax.rem(core + dc, 2))
    kinds, m_in, cols_in = wi.shape
    m_out, cols_out = wo.shape
    half_in, half_out = cols_in // 2, cols_out // 2
    per_in, per_out = half_in // STRIPE, half_out // STRIPE
    n_in = kinds * per_in
    slots = dy.shape[0]

    def remote(src, dst, sems, peer):
        return pltpu.make_async_remote_copy(src_ref=src, dst_ref=dst, send_sem=sems.at[0], recv_sem=sems.at[1],
                                            device_id=(peer,), device_id_type=MESH)

    def to_all(src, dst, sems):
        for peer in peers:
            remote(src, dst, sems, peer).start()

    def wait_for(ref, sem):
        pltpu.make_async_copy(ref, ref, sem).wait()

    def out_copy(s):
        cols = pl.ds(pl.multiple_of(core * half_out + s * STRIPE, LANES), STRIPE)
        return pltpu.make_async_copy(dyo_hbm.at[:, cols], dy.at[s], dy_sem.at[s])

    def in_copy(t):
        slot = lax.rem(t + per_out, slots)
        cols = pl.ds(pl.multiple_of(core * half_in + lax.rem(t, per_in) * STRIPE, LANES), STRIPE)
        return pltpu.make_async_copy(dyi_hbm.at[t // per_in, :, cols], dy.at[slot], dy_sem.at[slot])

    barrier = pltpu.get_barrier_semaphore()
    x_copy = pltpu.make_async_copy(x_hbm, xs.at[pl.ds(0, m_in)], x_sem.at[0])
    h_copy = pltpu.make_async_copy(h_hbm, hs.at[pl.ds(0, m_out)], x_sem.at[1])
    x_copy.start()
    h_copy.start()
    for peer in peers:
        pl.semaphore_signal(barrier, inc=1, device_id=(peer,), device_id_type=MESH)
    for s in range(per_out):
        out_copy(s).start()
    small = [pltpu.make_async_copy(src, dst, small_sem.at[i]) for i, (src, dst) in enumerate(
        ((ri_hbm, ri), (ci_hbm, ci), (ro_hbm, ro), (co_hbm, co), (beta_hbm, beta), (step_hbm, step), (rms_hbm, rms), (norm_hbm, norm)))]
    for copy in small:
        copy.start()
    for t in range(slots - per_out):
        in_copy(t).start()
    x_copy.wait()
    h_copy.wait()
    pl.semaphore_wait(barrier, n - 1)
    x_send = remote(xs.at[pl.ds(0, m_in)], xs.at[pl.ds(m_in, m_in)], xs_sem.at[0], partner)
    h_send = remote(hs.at[pl.ds(0, m_out)], hs.at[pl.ds(m_out, m_out)], xs_sem.at[1], partner)
    x_send.start()
    h_send.start()

    def put_cols(index, col_sq, add):
        for r in range(BLOCKS):
            part = col_sq[:, r * LANES:(r + 1) * LANES]
            where = (index + r // 2, pl.ds(r % 2, 1), slice(None))
            csend[where] = csend[where] + part if add else part

    def to_owner(p):
        for h in range(2):
            owner = 2 * p + h

            @pl.when(chip != owner)
            def _():
                remote(csend.at[owner], rs_land.at[chip], rs_sem, 2 * owner + core).start()

            @pl.when(chip == owner)
            def _():
                rs_land[chip] = csend[owner]

    for s in range(per_out):
        out_copy(s).wait()
        own = jnp.dot(hs[0:m_out, :], dy[s], preferred_element_type=F32)
        go[s, core] = own
        put_cols(2 * s, jnp.sum(own * own, axis=0, keepdims=True), False)
    for copy in small:
        copy.wait()
    lane = lax.broadcasted_iota(jnp.int32, (1, LANES), 1)

    def pack(values):
        row = jnp.zeros((1, LANES), F32)
        for i, value in enumerate(values):
            row = jnp.where(lane == i, value, row)
        return row

    ag_send[3:4, :] = jnp.zeros((1, LANES), F32)
    ag_send[2:3, :] = pack([jnp.sum(ri[k:k + 1, :], axis=1, keepdims=True) for k in range(kinds)]
                           + [jnp.sum(ro[...], axis=1, keepdims=True)])
    x_send.wait_recv()
    h_send.wait_recv()
    for s in range(per_out):
        other = jnp.dot(hs[m_out:2 * m_out, :], dy[s], preferred_element_type=F32)
        so[s] = other
        remote(so.at[s], go.at[s, core], g_sem.at[0], partner).start()
        put_cols(2 * s, jnp.sum(other * other, axis=0, keepdims=True), True)
        to_owner(s)
    for t in range(slots - per_out, n_in):
        in_copy(t).start()

    def in_step(t, carry):
        in_copy(t).wait()
        p = t + per_out
        both = jnp.dot(xs[...], dy[lax.rem(p, slots)], preferred_element_type=F32)
        gi[t, core] = both[0:m_in]
        si[t] = both[m_in:2 * m_in]
        remote(si.at[t], gi.at[t, core], g_sem.at[1], partner).start()
        put_cols(2 * p, jnp.sum(both * both, axis=0, keepdims=True), False)

        @pl.when(p < EARLY)
        def _():
            to_owner(p)

        @pl.when(p >= EARLY)
        def _():
            to_all(csend.at[pl.ds(2 * p, 2)], late_land.at[p - EARLY, me], late_sem)
            late_land[p - EARLY, me] = csend[pl.ds(2 * p, 2)]

        @pl.when(t == n_in - 2)
        def _():
            wait_for(rs_land.at[pl.ds(0, n // 2 - 1)], rs_sem.at[1])
            ag_send[0:2, :] = jnp.sum(rs_land[...], axis=0)
            to_all(ag_send, ag_land.at[me], ag_sem)
            ag_land[me] = ag_send[...]

        return carry

    lax.fori_loop(0, n_in, in_step, 0)
    wi_copy = pltpu.make_async_copy(wi_hbm, wi, w_sem.at[0])
    wo_copy = pltpu.make_async_copy(wo_hbm, wo, w_sem.at[1])
    wi_copy.start()
    wo_copy.start()

    wait_for(so, g_sem.at[0, 1])
    wait_for(si, g_sem.at[1, 1])

    def row_sq(ref, blocks):
        rows = ref.shape[2]

        def add(t, total):
            for c in range(2):
                for r in range(BLOCKS):
                    g = ref[t, c, :, r * LANES:(r + 1) * LANES]
                    total = total + g * g
            return total

        return jnp.sum(lax.fori_loop(blocks[0], blocks[1], add, jnp.zeros((rows, LANES), F32)), axis=1, keepdims=True)

    row_sums = [row_sq(gi, (k * per_in, (k + 1) * per_in)) for k in range(kinds)] + [row_sq(go, (0, per_out))]
    wi_copy.wait()
    wo_copy.wait()
    w_sums = [jnp.sum(wi[k] * wi[k], axis=(0, 1), keepdims=True) for k in range(kinds)]
    w_sums.append(jnp.sum(wo[...] * wo[...], axis=(0, 1), keepdims=True))

    wait_for(ag_land.at[pl.ds(0, n - 1)], ag_sem.at[1])
    wait_for(late_land.at[:, pl.ds(0, n - 1)], late_sem.at[1])
    for c in range(2):
        for q in range(2 * EARLY):
            csum[c, q] = ag_land[2 * q + c, 0:2, :]
        for stripe in range(LATE):
            total = late_land[stripe, c]
            for q in range(1, n // 2):
                total = total + late_land[stripe, 2 * q + c]
            csum[c, pl.ds(2 * (EARLY + stripe), 2)] = total
    misc = ag_land[0, 2:3, :]
    for d in range(1, n):
        misc = misc + ag_land[d, 2:3, :]

    def at_lane(row, i):
        return jnp.sum(jnp.where(lane == i, row, 0.0), axis=1, keepdims=True)

    first = [2 * (per_out + k * per_in) for k in range(kinds)] + [0]
    count = [2 * per_in] * kinds + [2 * per_out]
    rows_of = [m_in * n] * kinds + [m_out * n]
    cols_of = [cols_in] * kinds + [cols_out]
    grand = []
    for i in range(kinds + 1):
        part = jnp.sum(csum[:, first[i]:first[i] + count[i]], axis=(0, 1))
        grand.append(jnp.sum(part, axis=(0, 1), keepdims=True))
    norm_sq = grand[0]
    for g in grand[1:]:
        norm_sq = norm_sq + g
    scale = jnp.minimum(1.0, norm[...] / jnp.sqrt(norm_sq))
    keep = beta[...]
    mix = 1.0 - keep

    for i in range(kinds + 1):
        rows = m_out if i == kinds else m_in
        level = keep * (at_lane(misc, i) / rows_of[i]) + mix * (scale * (scale * (grand[i] / (rows_of[i] * cols_of[i]))) + EPS_ONE)
        eye = lax.broadcasted_iota(jnp.int32, (rows, rows), 0) == lax.broadcasted_iota(jnp.int32, (rows, rows), 1)
        old = ro[...] if i == kinds else ri[i:i + 1, :]
        old = jnp.sum(jnp.where(eye, old, 0.0), axis=1, keepdims=True)
        new = keep * old + mix * (scale * (scale * (row_sums[i] / cols_of[i])) + EPS_ONE)
        factor = jnp.broadcast_to(scale * lax.rsqrt(new / level), (rows, LANES))
        flat = jnp.sum(jnp.where(eye, new, 0.0), axis=0, keepdims=True)
        if i == kinds:
            ao[...] = factor
            ro_new[...] = flat
        else:
            ai[i] = factor
            ri_new[i:i + 1, :] = flat

    for c in range(2):
        for p in range(per_out + n_in):
            for r in range(BLOCKS):
                where = (c, 2 * p + r // 2, pl.ds(r % 2, 1), slice(None))
                if p < per_out:
                    i = kinds
                    spot = (pl.ds((c * half_out + p * STRIPE) // LANES + r, 1), slice(None))
                    old, store = co, co_new
                else:
                    i, s = divmod(p - per_out, per_in)
                    spot = (pl.ds(i, 1), pl.ds(c * half_in + s * STRIPE + r * LANES, LANES))
                    old, store = ci, ci_new
                new = keep * old[spot] + mix * (scale * (scale * (csum[where] / rows_of[i])) + EPS_ONE)
                store[spot] = new
                colf[where] = lax.rsqrt(new)

    def update(ref, factor, p0, blocks):
        def step_(t, total):
            for c in range(2):
                for r in range(BLOCKS):
                    col = colf[c, 2 * (p0 + t) + r // 2, pl.ds(r % 2, 1), :]
                    u = ref[t, c, :, r * LANES:(r + 1) * LANES] * factor * col
                    ref[t, c, :, r * LANES:(r + 1) * LANES] = u
                    total = total + u * u
            return total

        total = lax.fori_loop(blocks[0], blocks[1], step_, jnp.zeros(factor.shape, F32))
        return jnp.sum(total, axis=(0, 1), keepdims=True)

    u_sums = [update(gi, ai[k], per_out, (k * per_in, (k + 1) * per_in)) for k in range(kinds)]
    u_sums.append(update(go, ao[...], 0, (0, per_out)))
    fsend[...] = pack(u_sums + w_sums)
    to_all(fsend, f_land.at[me], f_sem)
    f_land[me] = fsend[...]
    wait_for(f_land.at[pl.ds(0, n - 1)], f_sem.at[1])
    sums = f_land[0]
    for d in range(1, n):
        sums = sums + f_land[d]
    for i in range(kinds + 1):
        size = float(rows_of[i] * cols_of[i])
        clip = jnp.maximum(1.0, jnp.sqrt(at_lane(sums, i) / size) / rms[...])
        move = step[...] * jnp.maximum(EPS_TWO, jnp.sqrt(at_lane(sums, kinds + 1 + i) / size))
        coef[i:i + 1, :] = jnp.broadcast_to(move / clip, (1, LANES))

    x_send.wait_send()
    h_send.wait_send()
    wait_for(so, g_sem.at[0, 0])
    wait_for(si, g_sem.at[1, 0])
    wait_for(rs_land.at[pl.ds(0, n // 2 - 1)], rs_sem.at[0])
    wait_for(ag_land.at[pl.ds(0, n - 1)], ag_sem.at[0])
    wait_for(late_land.at[:, pl.ds(0, n - 1)], late_sem.at[0])
    wait_for(f_land.at[pl.ds(0, n - 1)], f_sem.at[0])


def apply_kernel(gi, go, wi, wo, ri, ci, ro, co, coef, wi_out, ri_out, ci_out, wo_out, ro_out, co_out, wi_new, wo_new, sems):
    kinds, m_in, cols_in = wi.shape
    per_in, per_out = gi.shape[0] // kinds, go.shape[0]
    copies = []

    def send(src, dst):
        copies.append(pltpu.make_async_copy(src, dst, sems.at[len(copies)]))
        copies[-1].start()

    send(ri, ri_out)
    send(ci, ci_out)
    send(ro, ro_out)
    send(co, co_out)
    for k in range(kinds):
        for c in range(2):
            for s in range(per_in):
                cols = pl.ds(c * (cols_in // 2) + s * STRIPE, STRIPE)
                wi_new[k, :, cols] = wi[k, :, cols] - coef[k:k + 1, 0:1] * gi[k * per_in + s, c]
            part = pl.ds(c * (cols_in // 2), cols_in // 2)
            send(wi_new.at[k, :, part], wi_out.at[k, :, part])
    half = wo.shape[1] // 2
    for c in range(2):
        for s in range(per_out):
            cols = pl.ds(c * half + s * STRIPE, STRIPE)
            wo_new[:, cols] = wo[:, cols] - coef[kinds:kinds + 1, 0:1] * go[s, c]
        part = pl.ds(c * half, half)
        send(wo_new.at[:, part], wo_out.at[:, part])
    for copy in copies:
        copy.wait()


def solution(mesh):
    n = mesh.shape['tp']

    def local_step(x_norm, hid_act, dy_in, dy_out, w_in, w_out, row_in, col_in, row_out, col_out, beta_two, rel_step, clip_rms, clip_norm):
        kinds, m_in, cols_in = w_in.shape
        m_out, cols_out = w_out.shape
        tokens = x_norm.shape[0]
        n_in, n_out = kinds * cols_in // (2 * STRIPE), cols_out // (2 * STRIPE)
        stripes = n_in + n_out
        assert stripes == EARLY + LATE and n == 2 * 2 * EARLY
        slots = 10
        ins = [x_norm.T, hid_act.T, dy_in, dy_out, w_in, w_out, row_in, col_in, row_out.reshape(1, -1), col_out.reshape(-1, LANES)]
        ins += [v.reshape(1, 1) for v in (beta_two, rel_step, clip_rms, clip_norm)]
        outs = [(n_in, 2, m_in, STRIPE), (n_out, 2, m_out, STRIPE), w_in.shape, w_out.shape, row_in.shape, col_in.shape,
                (1, m_out), (cols_out // LANES, LANES), (8, LANES)]
        vmem = [((2 * m_in, tokens), jnp.bfloat16), ((2 * m_out, tokens), jnp.bfloat16), ((slots, tokens, STRIPE), jnp.bfloat16),
                ((n_in, m_in, STRIPE), F32), ((n_out, m_out, STRIPE), F32), ((2 * stripes, 2, LANES), F32),
                ((n // 2, 2, LANES), F32), ((4, LANES), F32), ((n, 4, LANES), F32), ((LATE, n, 2, 2, LANES), F32),
                ((2, 2 * stripes, 2, LANES), F32), ((2, 2 * stripes, 2, LANES), F32),
                ((kinds, m_in, LANES), F32), ((m_out, LANES), F32), ((1, LANES), F32), ((n, 1, LANES), F32),
                (row_in.shape, F32), (col_in.shape, F32), ((1, m_out), F32), ((cols_out // LANES, LANES), F32)]
        vmem += [((1, 1), F32)] * 4
        sems = [(slots,), (2,), (2,), (8,), (2, 2), (2, 2), (2,), (2,), (2,), (2,)]
        anywhere = pl.BlockSpec(memory_space=pl.ANY)
        inside = pl.BlockSpec(memory_space=pltpu.VMEM)
        mid = pl.pallas_call(
            lambda *refs: grads_kernel(n, *refs),
            out_shape=[pltpu.VMEM(s, F32) for s in outs],
            in_specs=[anywhere] * len(ins),
            out_specs=[inside] * len(outs),
            scratch_shapes=[pltpu.VMEM(*v) for v in vmem] + [pltpu.SemaphoreType.DMA(s) for s in sems],
            compiler_params=pltpu.CompilerParams(collective_id=0, has_side_effects=True, vmem_limit_bytes=56 * 2**20),
            name='grads',
        )(*ins)
        finals = [w_in.shape, row_in.shape, col_in.shape, w_out.shape, (1, m_out), (cols_out // LANES, LANES)]
        new = pl.pallas_call(
            apply_kernel,
            out_shape=[jax.ShapeDtypeStruct(s, F32) for s in finals],
            in_specs=[inside] * len(mid),
            out_specs=[anywhere] * len(finals),
            scratch_shapes=[pltpu.VMEM(w_in.shape, F32), pltpu.VMEM(w_out.shape, F32), pltpu.SemaphoreType.DMA((10,))],
            compiler_params=pltpu.CompilerParams(vmem_limit_bytes=8 * 2**20),
            name='apply',
        )(*mid)
        return (new[0], new[1], new[2], new[3], new[4].reshape(m_out), new[5].reshape(cols_out))

    in_specs = (P(None, 'tp'), P(None, 'tp'), P(), P(), P(None, 'tp', None), P('tp', None),
                P(None, 'tp'), P(), P('tp'), P(), P(), P(), P(), P())
    out_specs = (P(None, 'tp', None), P(None, 'tp'), P(), P('tp', None), P('tp'), P())
    return jax.shard_map(local_step, mesh=mesh, in_specs=in_specs, out_specs=out_specs, check_vma=False)
```

```python
import jax
import jax.numpy as jnp
from jax import lax
from jax.experimental import pallas as pl
from jax.experimental.pallas import tpu as pltpu
from jax.sharding import PartitionSpec as P

EPS_ONE = 1e-30
EPS_TWO = 1e-3
LANES = 128
STRIPE = 512
HALF = STRIPE // 2
LAST = 2
F32 = jnp.float32
MESH = pl.DeviceIdType.MESH


def grads_kernel(n, x_hbm, h_hbm, dyi_hbm, dyo_hbm, wi_hbm, wo_hbm, ri_hbm, ci_hbm, ro_hbm, co_hbm,
                 scal_hbm,
                 gi, go, wi, wo, ri_new, ci_new, ro_new, co_new, coef, ai, ao, colf,
                 xs, hs, dy, si, so, csend, land, misc_land, last_land, csum,
                 fsend, f_land, ri, ci, ro, co, scal,
                 dy_sem, x_sem, w_sem, small_sem, xs_sem, g_sem, land_sem, misc_sem, last_sem, fwd_sem, f_sem):
    me = lax.axis_index('tp')
    core = lax.rem(me, 2)
    chip = me // 2
    x, y, z = lax.rem(chip, 2), lax.rem(chip // 2, 2), chip // 4
    partner = me + 1 - 2 * core
    peers = {0: [], 1: []}
    for dz in (2, 1, 3, 0):
        for dy_ in (1, 0):
            for dx in (1, 0):
                for dc in (0, 1):
                    if dz or dy_ or dx or dc:
                        peers[dc].append(((lax.rem(z + dz, n // 8) * 2 + lax.rem(y + dy_, 2)) * 2 + lax.rem(x + dx, 2)) * 2
                                         + lax.rem(core + dc, 2))
    same = peers[0]
    everyone = [p for pair in zip(peers[0] + [None], peers[1]) for p in pair if p is not None]
    kinds, m_in, cols_in = wi.shape
    m_out, cols_out = wo.shape
    half_in, half_out = cols_in // 2, cols_out // 2
    per_in, per_out = half_in // STRIPE, half_out // STRIPE
    n_in = kinds * per_in
    stripes = n_in + per_out
    slots = dy.shape[0]
    early = land.shape[0]

    def remote(src, dst, sems, peer):
        return pltpu.make_async_remote_copy(src_ref=src, dst_ref=dst, send_sem=sems.at[0], recv_sem=sems.at[1],
                                            device_id=(peer,), device_id_type=MESH)

    def to_all(src, dst, sems, who):
        for peer in who:
            remote(src, dst, sems, peer).start()

    def wait_for(ref, sem):
        pltpu.make_async_copy(ref, ref, sem).wait()

    def out_copy(s):
        cols = pl.ds(pl.multiple_of(core * half_out + s * STRIPE, LANES), STRIPE)
        return pltpu.make_async_copy(dyo_hbm.at[:, cols], dy.at[s], dy_sem.at[s])

    def in_copy(t):
        slot = lax.rem(t + per_out, slots)
        cols = pl.ds(pl.multiple_of(core * half_in + lax.rem(t, per_in) * STRIPE, LANES), STRIPE)
        return pltpu.make_async_copy(dyi_hbm.at[t // per_in, :, cols], dy.at[slot], dy_sem.at[slot])

    barrier = pltpu.get_barrier_semaphore()
    x_copy = pltpu.make_async_copy(x_hbm, xs.at[pl.ds(0, m_in)], x_sem.at[0])
    h_copy = pltpu.make_async_copy(h_hbm, hs.at[pl.ds(0, m_out)], x_sem.at[1])
    x_copy.start()
    h_copy.start()
    out_copy(0).start()
    for peer in everyone:
        pl.semaphore_signal(barrier, inc=1, device_id=(peer,), device_id_type=MESH)
    for s in range(1, per_out):
        out_copy(s).start()
    small = [pltpu.make_async_copy(src, dst, small_sem.at[i]) for i, (src, dst) in enumerate(
        ((ri_hbm, ri), (ci_hbm, ci), (ro_hbm, ro), (co_hbm, co), (scal_hbm, scal)))]
    for copy in small:
        copy.start()

    def put_cols(p, h, col_sq, add):
        for r in range(2):
            part = col_sq[:, r * LANES:(r + 1) * LANES]
            where = (1 + 2 * p + h, pl.ds(r, 1), slice(None))
            csend[where] = csend[where] + part if add else part

    def share(p):
        mine = csend.at[pl.ds(1 + 2 * p, 2)]
        to_all(mine, land.at[p, chip], land_sem, same)
        land[p, chip] = mine[...]

    x_copy.wait()
    h_copy.wait()
    in_copy(0).start()
    in_copy(1).start()
    pl.semaphore_wait(barrier, n - 1)
    h_send = remote(hs.at[pl.ds(0, m_out)], hs.at[pl.ds(m_out, m_out)], xs_sem.at[1], partner)
    x_send = remote(xs.at[pl.ds(0, m_in)], xs.at[pl.ds(m_in, m_in)], xs_sem.at[0], partner)
    h_send.start()
    x_send.start()

    for s in range(per_out):
        out_copy(s).wait()
        in_copy(s + 2).start()
        for h in range(2):
            cols = pl.ds(h * HALF, HALF)
            own = jnp.dot(hs[0:m_out, :], dy[s, :, cols], preferred_element_type=F32)
            go[s, core, :, cols] = own
            put_cols(s, h, jnp.sum(own * own, axis=0, keepdims=True), False)
    in_copy(4).start()
    for copy in small:
        copy.wait()
    lane = lax.broadcasted_iota(jnp.int32, (1, LANES), 1)

    def pack(values):
        row = jnp.zeros((1, LANES), F32)
        for i, value in enumerate(values):
            row = jnp.where(lane == i, value, row)
        return row

    csend[0, 1:2, :] = jnp.zeros((1, LANES), F32)
    csend[0, 0:1, :] = pack([jnp.sum(ri[k:k + 1, :], axis=1, keepdims=True) for k in range(kinds)]
                            + [jnp.sum(ro[...], axis=1, keepdims=True)]) + scal[0:1, :]
    to_all(csend.at[0], misc_land.at[chip], misc_sem, same)
    misc_land[chip] = csend[0]
    h_send.wait_recv()
    in_copy(5).start()
    ahead = 6
    for s in range(per_out):
        for h in range(2):
            cols = pl.ds(h * HALF, HALF)
            other = jnp.dot(hs[m_out:2 * m_out, :], dy[s, :, cols], preferred_element_type=F32)
            so[s, :, cols] = other
            put_cols(s, h, jnp.sum(other * other, axis=0, keepdims=True), True)
        remote(so.at[s], go.at[s, core], g_sem.at[0], partner).start()
        share(s)
    x_send.wait_recv()

    def in_step(t, carry):
        in_copy(t).wait()

        @pl.when(t + ahead < n_in)
        def _():
            in_copy(t + ahead).start()

        p = t + per_out
        slot = lax.rem(p, slots)
        for h in range(2):
            cols = pl.ds(h * HALF, HALF)
            both = jnp.dot(xs[...], dy[slot, :, cols], preferred_element_type=F32)
            gi[t, core, :, cols] = both[0:m_in]
            si[t, :, cols] = both[m_in:2 * m_in]
            put_cols(p, h, jnp.sum(both * both, axis=0, keepdims=True), False)

        @pl.when(p < early)
        def _():
            share(p)

        @pl.when(p >= early)
        def _():
            mine = csend.at[pl.ds(1 + 2 * p, 2)]
            to_all(mine, last_land.at[p - early, me], last_sem, everyone)
            last_land[p - early, me] = mine[...]

        remote(si.at[t], gi.at[t, core], g_sem.at[1], partner).start()
        return carry

    lax.fori_loop(0, n_in, in_step, 0)
    wi_copy = pltpu.make_async_copy(wi_hbm, wi, w_sem.at[0])
    wo_copy = pltpu.make_async_copy(wo_hbm, wo, w_sem.at[1])
    wi_copy.start()
    wo_copy.start()

    wait_for(so, g_sem.at[0, 1])
    wait_for(si, g_sem.at[1, 1])

    def row_sq(ref, blocks):
        rows = ref.shape[2]

        def add(t, total):
            for c in range(2):
                for r in range(STRIPE // LANES):
                    g = ref[t, c, :, r * LANES:(r + 1) * LANES]
                    total = total + g * g
            return total

        return jnp.sum(lax.fori_loop(blocks[0], blocks[1], add, jnp.zeros((rows, LANES), F32)), axis=1, keepdims=True)

    row_sums = [row_sq(gi, (k * per_in, (k + 1) * per_in)) for k in range(kinds)] + [row_sq(go, (0, per_out))]

    wait_for(misc_land.at[pl.ds(0, n // 2 - 1)], misc_sem.at[1])
    wait_for(land.at[:, pl.ds(0, n // 2 - 1)], land_sem.at[1])
    csum[core, 0] = jnp.sum(misc_land[...], axis=0)
    for p in range(early):
        csum[core, pl.ds(1 + 2 * p, 2)] = jnp.sum(land[p], axis=0)
    done = csum.at[core, pl.ds(0, 1 + 2 * early)]
    forward = remote(done, done, fwd_sem, partner)
    forward.start()
    wi_copy.wait()
    wo_copy.wait()
    w_sums = [jnp.sum(jnp.sum(wi[k] * wi[k], axis=0, keepdims=True), axis=1, keepdims=True) for k in range(kinds)]
    w_sums.append(jnp.sum(jnp.sum(wo[...] * wo[...], axis=0, keepdims=True), axis=1, keepdims=True))
    forward.wait_recv()
    first = [1 + 2 * (per_out + k * per_in) for k in range(kinds)] + [1]
    count = [2 * per_in] * kinds + [2 * per_out]
    rows_of = [m_in * n] * kinds + [m_out * n]
    cols_of = [cols_in] * kinds + [cols_out]

    def at_lane(row, i):
        return jnp.sum(jnp.where(lane == i, row, 0.0), axis=1, keepdims=True)

    misc = csum[0, 0, 0:1, :] + csum[1, 0, 0:1, :]
    keep, norm, step, rms = (at_lane(misc, kinds + 1 + i) for i in range(4))
    mix = 1.0 - keep
    eyes, olds, levels, grand = [], [], [], []
    for i in range(kinds + 1):
        rows = m_out if i == kinds else m_in
        eyes.append(lax.broadcasted_iota(jnp.int32, (rows, rows), 0) == lax.broadcasted_iota(jnp.int32, (rows, rows), 1))
        old = ro[...] if i == kinds else ri[i:i + 1, :]
        olds.append(keep * jnp.sum(jnp.where(eyes[i], old, 0.0), axis=1, keepdims=True))
        levels.append(keep * (at_lane(misc, i) / rows_of[i]))
        known = min(first[i] + count[i], 1 + 2 * early)
        grand.append(jnp.sum(csum[:, first[i]:known], axis=(0, 1)))
    wait_for(last_land.at[:, pl.ds(0, n - 1)], last_sem.at[1])
    for stripe in range(stripes - early):
        for c in range(2):
            total = last_land[stripe, c]
            for q in range(1, n // 2):
                total = total + last_land[stripe, 2 * q + c]
            csum[c, pl.ds(1 + 2 * (early + stripe), 2)] = total
            grand[kinds - 1] = grand[kinds - 1] + jnp.sum(total, axis=0)
    grand = [jnp.sum(jnp.sum(g, axis=0, keepdims=True), axis=1, keepdims=True) for g in grand]
    norm_sq = grand[0]
    for g in grand[1:]:
        norm_sq = norm_sq + g
    scale = jnp.minimum(1.0, norm / jnp.sqrt(norm_sq))

    for i in range(kinds + 1):
        rows = m_out if i == kinds else m_in
        level = levels[i] + mix * (scale * (scale * (grand[i] / (rows_of[i] * cols_of[i]))) + EPS_ONE)
        new = olds[i] + mix * (scale * (scale * (row_sums[i] / cols_of[i])) + EPS_ONE)
        factor = jnp.broadcast_to(scale * lax.rsqrt(new / level), (rows, LANES))
        if i == kinds:
            ao[...] = factor
        else:
            ai[i] = factor
        olds[i] = new

    for c in range(2):
        for p in range(stripes):
            for r in range(STRIPE // LANES):
                where = (c, 1 + 2 * p + r // 2, pl.ds(r % 2, 1), slice(None))
                if p < per_out:
                    i = kinds
                    spot = (pl.ds((c * half_out + p * STRIPE) // LANES + r, 1), slice(None))
                    old, store = co, co_new
                else:
                    i, s = divmod(p - per_out, per_in)
                    spot = (pl.ds(i, 1), pl.ds(c * half_in + s * STRIPE + r * LANES, LANES))
                    old, store = ci, ci_new
                new = keep * old[spot] + mix * (scale * (scale * (csum[where] / rows_of[i])) + EPS_ONE)
                store[spot] = new
                colf[c, STRIPE // LANES * p + r] = lax.rsqrt(new)

    def update_sq(ref, factor, p0, blocks):
        rows = ref.shape[2]

        def add(t, total):
            for c in range(2):
                for r in range(STRIPE // LANES):
                    part = ref[t, c, :, r * LANES:(r + 1) * LANES] * factor
                    part = part * part
                    fold = part[0:8]
                    for b in range(1, rows // 8):
                        fold = fold + part[8 * b:8 * (b + 1)]
                    col = colf[c, STRIPE // LANES * (p0 + t) + r]
                    total = total + fold * (col * col)
            return total

        total = lax.fori_loop(blocks[0], blocks[1], add, jnp.zeros((8, LANES), F32))
        return jnp.sum(jnp.sum(total, axis=0, keepdims=True), axis=1, keepdims=True)

    u_sums = [update_sq(gi, ai[k], per_out, (k * per_in, (k + 1) * per_in)) for k in range(kinds)]
    u_sums.append(update_sq(go, ao[...], 0, (0, per_out)))
    fsend[...] = pack(u_sums + w_sums)
    to_all(fsend, f_land.at[me], f_sem, everyone)
    f_land[me] = fsend[...]

    for i in range(kinds + 1):
        flat = jnp.sum(jnp.where(eyes[i], olds[i], 0.0), axis=0, keepdims=True)
        if i == kinds:
            ro_new[...] = flat
        else:
            ri_new[i:i + 1, :] = flat

    x_send.wait_send()
    h_send.wait_send()
    forward.wait_send()
    wait_for(so, g_sem.at[0, 0])
    wait_for(si, g_sem.at[1, 0])
    wait_for(misc_land.at[pl.ds(0, n // 2 - 1)], misc_sem.at[0])
    wait_for(land.at[:, pl.ds(0, n // 2 - 1)], land_sem.at[0])
    wait_for(last_land.at[:, pl.ds(0, n - 1)], last_sem.at[0])
    wait_for(f_land.at[pl.ds(0, n - 1)], f_sem.at[1])
    sums = f_land[0]
    for d in range(1, n):
        sums = sums + f_land[d]
    for i in range(kinds + 1):
        size = float(rows_of[i] * cols_of[i])
        clip = jnp.maximum(1.0, jnp.sqrt(at_lane(sums, i) / size) / rms)
        move = step * jnp.maximum(EPS_TWO, jnp.sqrt(at_lane(sums, kinds + 1 + i) / size))
        coef[i:i + 1, :] = jnp.broadcast_to(move / clip, (1, LANES))
    wait_for(f_land.at[pl.ds(0, n - 1)], f_sem.at[0])


def scalars_kernel(first, *refs):
    lane = lax.broadcasted_iota(jnp.int32, (8, LANES), 1)
    row = jnp.zeros((8, LANES), F32)
    for i, ref in enumerate(refs[:-1]):
        row = jnp.where(lane == first + i, ref[...], row)
    refs[-1][...] = row


def apply_kernel(gi, go, wi, wo, ri, ci, ro, co, coef, ai, ao, colf, wi_out, ri_out, ci_out, wo_out, ro_out, co_out, wi_new, wo_new, sems):
    kinds, m_in, cols_in = wi.shape
    per_in, per_out = gi.shape[0] // kinds, go.shape[0]
    lanes = STRIPE // LANES
    copies = []

    def send(src, dst):
        copies.append(pltpu.make_async_copy(src, dst, sems.at[len(copies)]))
        copies[-1].start()

    def blocks(factor, g, p, c, old, new, out, first):
        for r in range(lanes):
            cols = pl.ds(first + r * LANES, LANES)
            new[:, cols] = old[:, cols] - (factor * colf[c, lanes * p + r]) * g[:, r * LANES:(r + 1) * LANES]
        part = pl.ds(first, STRIPE)
        send(new.at[:, part], out.at[:, part])

    for c in range(2):
        factor = ao[...] * coef[kinds:kinds + 1, :]
        for s in range(per_out):
            blocks(factor, go.at[s, c], s, c, wo, wo_new, wo_out, c * (wo.shape[1] // 2) + s * STRIPE)
    send(ri, ri_out)
    send(ci, ci_out)
    send(ro, ro_out)
    send(co, co_out)
    for k in range(kinds):
        factor = ai[k] * coef[k:k + 1, :]
        for c in range(2):
            for s in range(per_in):
                t = k * per_in + s
                blocks(factor, gi.at[t, c], per_out + t, c, wi.at[k], wi_new.at[k], wi_out.at[k], c * (cols_in // 2) + s * STRIPE)
    for copy in copies:
        copy.wait()


def solution(mesh):
    n = mesh.shape['tp']

    def local_step(x_norm, hid_act, dy_in, dy_out, w_in, w_out, row_in, col_in, row_out, col_out, beta_two, rel_step, clip_rms, clip_norm):
        kinds, m_in, cols_in = w_in.shape
        m_out, cols_out = w_out.shape
        tokens = x_norm.shape[0]
        inside = pl.BlockSpec(memory_space=pltpu.VMEM)
        scalars = lax.cond(
            lax.axis_index('tp') == 0,
            lambda *values: pl.pallas_call(
                lambda *refs: scalars_kernel(kinds + 1, *refs), out_shape=jax.ShapeDtypeStruct((8, LANES), F32),
                in_specs=[inside] * 4, out_specs=inside, name='scalars')(*[v.reshape(1, 1) for v in values]),
            lambda *values: jnp.zeros((8, LANES), F32),
            beta_two, clip_norm, rel_step, clip_rms)
        n_in, n_out = kinds * cols_in // (2 * STRIPE), cols_out // (2 * STRIPE)
        stripes = n_in + n_out
        early = stripes - LAST
        slots = 10
        ins = [x_norm.T, hid_act.T, dy_in, dy_out, w_in, w_out, row_in, col_in, row_out.reshape(1, -1), col_out.reshape(-1, LANES)]
        ins.append(scalars)
        outs = [(n_in, 2, m_in, STRIPE), (n_out, 2, m_out, STRIPE), w_in.shape, w_out.shape, row_in.shape, col_in.shape,
                (1, m_out), (cols_out // LANES, LANES), (8, LANES), (kinds, m_in, LANES), (m_out, LANES), (2, stripes * STRIPE // LANES, 1, LANES)]
        vmem = [((2 * m_in, tokens), jnp.bfloat16), ((2 * m_out, tokens), jnp.bfloat16), ((slots, tokens, STRIPE), jnp.bfloat16),
                ((n_in, m_in, STRIPE), F32), ((n_out, m_out, STRIPE), F32), ((1 + 2 * stripes, 2, LANES), F32),
                ((early, n // 2, 2, 2, LANES), F32), ((n // 2, 2, LANES), F32), ((LAST, n, 2, 2, LANES), F32), ((2, 1 + 2 * stripes, 2, LANES), F32),
                ((1, LANES), F32), ((n, 1, LANES), F32),
                (row_in.shape, F32), (col_in.shape, F32), ((1, m_out), F32), ((cols_out // LANES, LANES), F32)]
        vmem.append(((8, LANES), F32))
        sems = [(slots,), (2,), (2,), (5,), (2, 2), (2, 2), (2,), (2,), (2,), (2,), (2,)]
        anywhere = pl.BlockSpec(memory_space=pl.ANY)
        mid = pl.pallas_call(
            lambda *refs: grads_kernel(n, *refs),
            out_shape=[pltpu.VMEM(s, F32) for s in outs],
            in_specs=[anywhere] * len(ins),
            out_specs=[inside] * len(outs),
            scratch_shapes=[pltpu.VMEM(*v) for v in vmem] + [pltpu.SemaphoreType.DMA(s) for s in sems],
            compiler_params=pltpu.CompilerParams(collective_id=0, has_side_effects=True, vmem_limit_bytes=56 * 2**20),
            name='grads',
        )(*ins)
        finals = [w_in.shape, row_in.shape, col_in.shape, w_out.shape, (1, m_out), (cols_out // LANES, LANES)]
        new = pl.pallas_call(
            apply_kernel,
            out_shape=[jax.ShapeDtypeStruct(s, F32) for s in finals],
            in_specs=[inside] * len(mid),
            out_specs=[anywhere] * len(finals),
            scratch_shapes=[pltpu.VMEM(w_in.shape, F32), pltpu.VMEM(w_out.shape, F32), pltpu.SemaphoreType.DMA((2 * stripes + 4,))],
            compiler_params=pltpu.CompilerParams(vmem_limit_bytes=8 * 2**20),
            name='apply',
        )(*mid)
        return (new[0], new[1], new[2], new[3], new[4].reshape(m_out), new[5].reshape(cols_out))

    in_specs = (P(None, 'tp'), P(None, 'tp'), P(), P(), P(None, 'tp', None), P('tp', None),
                P(None, 'tp'), P(), P('tp'), P(), P(), P(), P(), P())
    out_specs = (P(None, 'tp', None), P(None, 'tp'), P(), P('tp', None), P('tp'), P())
    return jax.shard_map(local_step, mesh=mesh, in_specs=in_specs, out_specs=out_specs, check_vma=False)
```

```python
import jax
import jax.numpy as jnp
from jax import lax
from jax.experimental import pallas as pl
from jax.experimental.pallas import tpu as pltpu
from jax.sharding import PartitionSpec as P

EPS_ONE = 1e-30
EPS_TWO = 1e-3
LANES = 128
STRIPE = 512
HALF = STRIPE // 2
F32 = jnp.float32
MESH = pl.DeviceIdType.MESH


def grads_kernel(n, x_hbm, h_hbm, dyi_hbm, dyo_hbm, wi_hbm, wo_hbm, ri_hbm, ci_hbm, ro_hbm, co_hbm,
                 scal_hbm,
                 gi, go, wi, wo, ri_new, ci_new, ro_new, co_new, coef, ai, ao, colf,
                 xs, hs, dy, si, so, csend, land, mid_land, misc_land, last_land, csum, ri_sq, ro_sq, ri_got, ro_got, split,
                 fsend, f_land, ri, ci, ro, co, scal,
                 dy_sem, x_sem, w_sem, small_sem, xs_sem, g_sem, land_sem, mid_sem, misc_sem, last_sem, fwd_sem, row_sem, f_sem):
    me = lax.axis_index('tp')
    core = lax.rem(me, 2)
    chip = me // 2
    x, y, z = lax.rem(chip, 2), lax.rem(chip // 2, 2), chip // 4
    partner = me + 1 - 2 * core
    high = z // 2
    planes = [3 * (1 - high), 2 - high, z + 1 - 2 * lax.rem(z, 2), z]
    same, everyone = [], []
    for plane in planes:
        for far_y in (1, 0):
            for far_x in (1, 0):
                for other in (0, 1):
                    if plane is z and not (far_y or far_x or other):
                        continue
                    place = (plane * 2 + lax.rem(y + far_y, 2)) * 2 + lax.rem(x + far_x, 2)
                    everyone.append(2 * place + lax.rem(core + other, 2))
                    if not other:
                        same.append(everyone[-1])
    kinds, m_in, cols_in = wi.shape
    m_out, cols_out = wo.shape
    half_in, half_out = cols_in // 2, cols_out // 2
    per_in, per_out = half_in // STRIPE, half_out // STRIPE
    n_in = kinds * per_in
    stripes = n_in + per_out
    slots, tokens = dy.shape[0:2]
    early = 2 * land.shape[0]
    single = mid_land.shape[0]
    shared = early + single

    def remote(src, dst, sems, peer):
        return pltpu.make_async_remote_copy(src_ref=src, dst_ref=dst, send_sem=sems.at[0], recv_sem=sems.at[1],
                                            device_id=(peer,), device_id_type=MESH)

    def to_all(src, dst, sems, who):
        for peer in who:
            remote(src, dst, sems, peer).start()

    def wait_for(ref, sem):
        pltpu.make_async_copy(ref, ref, sem).wait()

    def out_copy(s):
        cols = pl.ds(pl.multiple_of(core * half_out + s * STRIPE, LANES), STRIPE)
        return pltpu.make_async_copy(dyo_hbm.at[:, cols], dy.at[s], dy_sem.at[s])

    def in_copy(t):
        slot = lax.rem(t + per_out, slots)
        cols = pl.ds(pl.multiple_of(core * half_in + lax.rem(t, per_in) * STRIPE, LANES), STRIPE)
        return pltpu.make_async_copy(dyi_hbm.at[t // per_in, :, cols], dy.at[slot], dy_sem.at[slot])

    def last_copy(part):
        t = n_in - 1
        slot = (t + per_out) % slots
        some = pl.ds(part * (tokens // 2), tokens // 2)
        cols = pl.ds(pl.multiple_of(core * half_in + t % per_in * STRIPE, LANES), STRIPE)
        return pltpu.make_async_copy(dyi_hbm.at[t // per_in, some, cols], dy.at[slot, some, :], dy_sem.at[slot + part * slots])

    barrier = pltpu.get_barrier_semaphore()
    x_copy = pltpu.make_async_copy(x_hbm, xs.at[pl.ds(0, m_in)], x_sem.at[0])
    h_copy = pltpu.make_async_copy(h_hbm, hs.at[pl.ds(0, m_out)], x_sem.at[1])
    x_copy.start()
    h_copy.start()
    out_copy(0).start()
    for peer in everyone:
        pl.semaphore_signal(barrier, inc=1, device_id=(peer,), device_id_type=MESH)
    for s in range(1, per_out):
        out_copy(s).start()
    small = [pltpu.make_async_copy(src, dst, small_sem.at[i]) for i, (src, dst) in enumerate(
        ((ri_hbm, ri), (ci_hbm, ci), (ro_hbm, ro), (co_hbm, co), (scal_hbm, scal)))]
    for copy in small:
        copy.start()

    def put_cols(p, h, col_sq, add):
        for r in range(2):
            part = col_sq[:, r * LANES:(r + 1) * LANES]
            where = (1 + 2 * p + h, pl.ds(r, 1), slice(None))
            csend[where] = csend[where] + part if add else part

    def share(pair):
        mine = csend.at[pl.ds(1 + 4 * pair, 4)]
        to_all(mine, land.at[pair, chip], land_sem, same)
        land[pair, chip] = mine[...]

    def add_rows(ref, where, sq):
        ref[where] = ref[where] + (sq[:, 0:LANES] + sq[:, LANES:HALF])

    ri_sq[...] = jnp.zeros_like(ri_sq)
    ro_sq[...] = jnp.zeros_like(ro_sq)
    x_copy.wait()
    h_copy.wait()
    in_copy(0).start()
    in_copy(1).start()
    in_copy(2).start()
    pl.semaphore_wait(barrier, n - 1)
    h_send = remote(hs.at[pl.ds(0, m_out)], hs.at[pl.ds(m_out, m_out)], xs_sem.at[1], partner)
    x_send = remote(xs.at[pl.ds(0, m_in)], xs.at[pl.ds(m_in, m_in)], xs_sem.at[0], partner)
    x_send.start()
    h_send.start()

    for s in range(per_out):
        out_copy(s).wait()
        in_copy(s + 3).start()
        for h in range(2):
            cols = pl.ds(h * HALF, HALF)
            own = jnp.dot(hs[0:m_out, :], dy[s, :, cols], preferred_element_type=F32)
            go[s, core, :, cols] = own
            own = own * own
            put_cols(s, h, jnp.sum(own, axis=0, keepdims=True), False)
            add_rows(ro_sq, (pl.ds(0, m_out), slice(None)), own)
    for copy in small:
        copy.wait()
    lane = lax.broadcasted_iota(jnp.int32, (1, LANES), 1)

    def pack(values):
        row = jnp.zeros((1, LANES), F32)
        for i, value in enumerate(values):
            row = jnp.where(lane == i, value, row)
        return row

    csend[0, 1:2, :] = jnp.zeros((1, LANES), F32)
    csend[0, 0:1, :] = pack([jnp.sum(ri[k:k + 1, :], axis=1, keepdims=True) for k in range(kinds)]
                            + [jnp.sum(ro[...], axis=1, keepdims=True)]) + scal[0:1, :]
    to_all(csend.at[0], misc_land.at[chip], misc_sem, same)
    misc_land[chip] = csend[0]
    x_send.wait_recv()
    in_copy(5).start()
    ahead = 6

    def partner_rows():
        h_send.wait_recv()
        for s in range(per_out):
            for h in range(2):
                cols = pl.ds(h * HALF, HALF)
                other = jnp.dot(hs[m_out:2 * m_out, :], dy[s, :, cols], preferred_element_type=F32)
                so[s, :, cols] = other
                other = other * other
                put_cols(s, h, jnp.sum(other, axis=0, keepdims=True), True)
                add_rows(ro_sq, (pl.ds(m_out, m_out), slice(None)), other)
        remote(so, go.at[:, core], g_sem.at[0], partner).start()
        remote(ro_sq.at[pl.ds(m_out, m_out)], ro_got, row_sem.at[0], partner).start()
        share(0)

    def product(t):
        p = t + per_out
        for h in range(2):
            cols = pl.ds(h * HALF, HALF)
            both = jnp.dot(xs[...], dy[lax.rem(p, slots), :, cols], preferred_element_type=F32)
            gi[t, core, :, cols] = both[0:m_in]
            si[t, :, cols] = both[m_in:2 * m_in]
            both = both * both
            put_cols(p, h, jnp.sum(both, axis=0, keepdims=True), False)
            add_rows(ri_sq, t // per_in, both)

    def give(t, size):
        remote(si.at[pl.ds(t, size)], gi.at[pl.ds(t, size), core], g_sem.at[1], partner).start()

    def in_step(i, carry):
        @pl.when(i == 1)
        def _():
            partner_rows()

        for t in (2 * i, 2 * i + 1):
            in_copy(t).wait()

            @pl.when(t + ahead < n_in - 1)
            def _():
                in_copy(t + ahead).start()

            @pl.when(t + ahead == n_in - 1)
            def _():
                for h in range(2):
                    last_copy(h).start()

        for t in (2 * i, 2 * i + 1):
            product(t)
        share(i + 1)
        give(2 * i, 2)
        return carry

    lax.fori_loop(0, early // 2 - 1, in_step, 0)
    def single_step(t, carry):
        in_copy(t).wait()
        product(t)
        p = t + per_out
        mine = csend.at[pl.ds(1 + 2 * p, 2)]
        to_all(mine, mid_land.at[p - early, chip], mid_sem, same)
        mid_land[p - early, chip] = mine[...]
        give(t, 1)
        return carry

    lax.fori_loop(early - per_out, n_in - 1, single_step, 0)
    t = n_in - 1
    last_copy(0).wait()
    for part in range(2):
        some = pl.ds(part * (tokens // 2), tokens // 2)
        if part:
            last_copy(1).wait()
            wi_copy = pltpu.make_async_copy(wi_hbm, wi, w_sem.at[0])
            wo_copy = pltpu.make_async_copy(wo_hbm, wo, w_sem.at[1])
            wi_copy.start()
            wo_copy.start()
        for h in range(2):
            cols = pl.ds(h * HALF, HALF)
            both = jnp.dot(xs[:, some], dy[(t + per_out) % slots, some, cols], preferred_element_type=F32)
            if not part:
                split[h] = both
                continue
            both = split[h] + both
            gi[t, core, :, cols] = both[0:m_in]
            si[t, :, cols] = both[m_in:2 * m_in]
            both = both * both
            put_cols(t + per_out, h, jnp.sum(both, axis=0, keepdims=True), False)
            add_rows(ri_sq, t // per_in, both)
    mine = csend.at[pl.ds(1 + 2 * shared, 2)]
    to_all(mine, last_land.at[me], last_sem, everyone)
    last_land[me] = mine[...]
    remote(ri_sq.at[:, pl.ds(m_in, m_in)], ri_got, row_sem.at[1], partner).start()
    give(n_in - 1, 1)
    wait_for(misc_land.at[pl.ds(0, n // 2 - 1)], misc_sem.at[1])
    wait_for(land.at[:, pl.ds(0, n // 2 - 1)], land_sem.at[1])
    csum[core, 0] = jnp.sum(misc_land[...], axis=0)
    for pair in range(early // 2):
        csum[core, pl.ds(1 + 4 * pair, 4)] = jnp.sum(land[pair], axis=0)
    wait_for(mid_land.at[:, pl.ds(0, n // 2 - 1)], mid_sem.at[1])
    for i in range(single):
        csum[core, pl.ds(1 + 2 * (early + i), 2)] = jnp.sum(mid_land[i], axis=0)
    done = csum.at[core, pl.ds(0, 1 + 2 * shared)]
    forward = remote(done, done, fwd_sem, partner)
    forward.start()
    wait_for(ro_got, row_sem.at[0, 1])
    wait_for(ri_got, row_sem.at[1, 1])
    row_sums = [jnp.sum(ri_sq[k, 0:m_in] + ri_got[k], axis=1, keepdims=True) for k in range(kinds)]
    row_sums.append(jnp.sum(ro_sq[0:m_out] + ro_got[...], axis=1, keepdims=True))
    def square_sum(ref, cols):
        rows = ref.shape[0]
        total = [jnp.zeros((8, LANES), F32) for _ in range(4)]
        for r in range(cols // LANES):
            for b in range(rows // 8):
                w = ref[8 * b:8 * (b + 1), r * LANES:(r + 1) * LANES]
                total[b % 4] = total[b % 4] + w * w
        total = (total[0] + total[1]) + (total[2] + total[3])
        return jnp.sum(jnp.sum(total, axis=0, keepdims=True), axis=1, keepdims=True)

    wi_copy.wait()
    wo_copy.wait()
    w_sums = [square_sum(wi.at[k], cols_in) for k in range(kinds)] + [square_sum(wo, cols_out)]
    forward.wait_recv()
    first = [1 + 2 * (per_out + k * per_in) for k in range(kinds)] + [1]
    count = [2 * per_in] * kinds + [2 * per_out]
    rows_of = [m_in * n] * kinds + [m_out * n]
    cols_of = [cols_in] * kinds + [cols_out]

    def at_lane(row, i):
        return jnp.sum(jnp.where(lane == i, row, 0.0), axis=1, keepdims=True)

    misc = csum[0, 0, 0:1, :] + csum[1, 0, 0:1, :]
    keep, norm, step, rms = (at_lane(misc, kinds + 1 + i) for i in range(4))
    mix = 1.0 - keep
    eyes, olds, levels, grand = [], [], [], []
    for i in range(kinds + 1):
        rows = m_out if i == kinds else m_in
        eyes.append(lax.broadcasted_iota(jnp.int32, (rows, rows), 0) == lax.broadcasted_iota(jnp.int32, (rows, rows), 1))
        old = ro[...] if i == kinds else ri[i:i + 1, :]
        olds.append(keep * jnp.sum(jnp.where(eyes[i], old, 0.0), axis=1, keepdims=True))
        levels.append(keep * (at_lane(misc, i) / rows_of[i]))
        known = min(first[i] + count[i], 1 + 2 * shared)
        grand.append(jnp.sum(csum[:, first[i]:known], axis=(0, 1)))
    wait_for(last_land.at[pl.ds(0, n - 1)], last_sem.at[1])
    for c in range(2):
        total = last_land[c]
        for q in range(1, n // 2):
            total = total + last_land[2 * q + c]
        csum[c, pl.ds(1 + 2 * shared, 2)] = total
        grand[kinds - 1] = grand[kinds - 1] + jnp.sum(total, axis=0)
    grand = [jnp.sum(jnp.sum(g, axis=0, keepdims=True), axis=1, keepdims=True) for g in grand]
    norm_sq = grand[0]
    for g in grand[1:]:
        norm_sq = norm_sq + g
    scale = jnp.minimum(1.0, norm / jnp.sqrt(norm_sq))

    for i in range(kinds + 1):
        rows = m_out if i == kinds else m_in
        level = levels[i] + mix * (scale * (scale * (grand[i] / (rows_of[i] * cols_of[i]))) + EPS_ONE)
        new = olds[i] + mix * (scale * (scale * (row_sums[i] / cols_of[i])) + EPS_ONE)
        factor = jnp.broadcast_to(scale * lax.rsqrt(new / level), (rows, LANES))
        if i == kinds:
            ao[...] = factor
        else:
            ai[i] = factor
        olds[i] = new

    for c in range(2):
        for p in range(stripes):
            for r in range(STRIPE // LANES):
                where = (c, 1 + 2 * p + r // 2, pl.ds(r % 2, 1), slice(None))
                if p < per_out:
                    i = kinds
                    spot = (pl.ds((c * half_out + p * STRIPE) // LANES + r, 1), slice(None))
                    old, store = co, co_new
                else:
                    i, s = divmod(p - per_out, per_in)
                    spot = (pl.ds(i, 1), pl.ds(c * half_in + s * STRIPE + r * LANES, LANES))
                    old, store = ci, ci_new
                new = keep * old[spot] + mix * (scale * (scale * (csum[where] / rows_of[i])) + EPS_ONE)
                store[spot] = new
                colf[c, STRIPE // LANES * p + r] = lax.rsqrt(new)

    wait_for(so, g_sem.at[0, 1])
    wait_for(si, g_sem.at[1, 1])
    def update_sq(ref, factor, p0, blocks):
        rows = ref.shape[2]

        def add(t, total):
            for c in range(2):
                for r in range(STRIPE // LANES):
                    part = ref[t, c, :, r * LANES:(r + 1) * LANES] * factor
                    part = part * part
                    fold = part[0:8]
                    for b in range(1, rows // 8):
                        fold = fold + part[8 * b:8 * (b + 1)]
                    col = colf[c, STRIPE // LANES * (p0 + t) + r]
                    total = total + fold * (col * col)
            return total

        total = lax.fori_loop(blocks[0], blocks[1], add, jnp.zeros((8, LANES), F32), unroll=True)
        return jnp.sum(jnp.sum(total, axis=0, keepdims=True), axis=1, keepdims=True)

    u_sums = [update_sq(gi, ai[k], per_out, (k * per_in, (k + 1) * per_in)) for k in range(kinds)]
    u_sums.append(update_sq(go, ao[...], 0, (0, per_out)))
    fsend[...] = pack(u_sums + w_sums)
    to_all(fsend, f_land.at[me], f_sem, everyone)
    f_land[me] = fsend[...]

    for i in range(kinds + 1):
        flat = jnp.sum(jnp.where(eyes[i], olds[i], 0.0), axis=0, keepdims=True)
        if i == kinds:
            ro_new[...] = flat
        else:
            ri_new[i:i + 1, :] = flat

    x_send.wait_send()
    h_send.wait_send()
    forward.wait_send()
    wait_for(so, g_sem.at[0, 0])
    wait_for(si, g_sem.at[1, 0])
    wait_for(misc_land.at[pl.ds(0, n // 2 - 1)], misc_sem.at[0])
    wait_for(land.at[:, pl.ds(0, n // 2 - 1)], land_sem.at[0])
    wait_for(mid_land.at[:, pl.ds(0, n // 2 - 1)], mid_sem.at[0])
    wait_for(ro_got, row_sem.at[0, 0])
    wait_for(ri_got, row_sem.at[1, 0])
    wait_for(last_land.at[pl.ds(0, n - 1)], last_sem.at[0])
    wait_for(f_land.at[pl.ds(0, n - 1)], f_sem.at[1])
    sums = f_land[0]
    for d in range(1, n):
        sums = sums + f_land[d]
    for i in range(kinds + 1):
        size = float(rows_of[i] * cols_of[i])
        clip = jnp.maximum(1.0, jnp.sqrt(at_lane(sums, i) / size) / rms)
        move = step * jnp.maximum(EPS_TWO, jnp.sqrt(at_lane(sums, kinds + 1 + i) / size))
        coef[i:i + 1, :] = jnp.broadcast_to(move / clip, (1, LANES))
    wait_for(f_land.at[pl.ds(0, n - 1)], f_sem.at[0])


def scalar_kernel(place, one, two, row):
    lane = lax.broadcasted_iota(jnp.int32, (8, LANES), 1)
    row[...] = jnp.where(lane == place, one[...], jnp.where(lane == place + 1, two[...], 0.0))


def apply_kernel(gi, go, wi, wo, ri, ci, ro, co, coef, ai, ao, colf, wi_out, ri_out, ci_out, wo_out, ro_out, co_out, wi_new, wo_new, sems):
    kinds, m_in, cols_in = wi.shape
    per_in, per_out = gi.shape[0] // kinds, go.shape[0]
    lanes = STRIPE // LANES
    copies = []

    def send(src, dst):
        copies.append(pltpu.make_async_copy(src, dst, sems.at[len(copies)]))
        copies[-1].start()

    def blocks(factor, g, p, c, old, new, out, first):
        for r in range(lanes):
            cols = pl.ds(first + r * LANES, LANES)
            new[:, cols] = old[:, cols] - (factor * colf[c, lanes * p + r]) * g[:, r * LANES:(r + 1) * LANES]
        part = pl.ds(first, STRIPE)
        send(new.at[:, part], out.at[:, part])

    for c in range(2):
        factor = ao[...] * coef[kinds:kinds + 1, :]
        for s in range(per_out):
            blocks(factor, go.at[s, c], s, c, wo, wo_new, wo_out, c * (wo.shape[1] // 2) + s * STRIPE)
    send(ri, ri_out)
    send(ci, ci_out)
    send(ro, ro_out)
    send(co, co_out)
    for k in range(kinds):
        factor = ai[k] * coef[k:k + 1, :]
        for c in range(2):
            for s in range(per_in):
                t = k * per_in + s
                blocks(factor, gi.at[t, c], per_out + t, c, wi.at[k], wi_new.at[k], wi_out.at[k], c * (cols_in // 2) + s * STRIPE)
    for copy in copies:
        copy.wait()


def solution(mesh):
    n = mesh.shape['tp']

    def local_step(x_norm, hid_act, dy_in, dy_out, w_in, w_out, row_in, col_in, row_out, col_out, beta_two, rel_step, clip_rms, clip_norm):
        kinds, m_in, cols_in = w_in.shape
        m_out, cols_out = w_out.shape
        tokens = x_norm.shape[0]
        inside = pl.BlockSpec(memory_space=pltpu.VMEM)
        scalars = lax.switch(
            jnp.minimum(lax.axis_index('tp'), 2),
            [lambda *values, i=i: pl.pallas_call(
                lambda *refs: scalar_kernel(kinds + 1 + 2 * i, *refs), out_shape=jax.ShapeDtypeStruct((8, LANES), F32),
                in_specs=[inside] * 2, out_specs=inside, name='scalar')(*[v.reshape(1, 1) for v in values[2 * i:2 * i + 2]]) for i in range(2)]
            + [lambda *values: jnp.zeros((8, LANES), F32)],
            beta_two, clip_norm, rel_step, clip_rms)
        n_in, n_out = kinds * cols_in // (2 * STRIPE), cols_out // (2 * STRIPE)
        stripes = n_in + n_out
        single = 3
        early = stripes - single - 1
        slots = 10
        ins = [x_norm.T, hid_act.T, dy_in, dy_out, w_in, w_out, row_in, col_in, row_out.reshape(1, -1), col_out.reshape(-1, LANES)]
        ins.append(scalars)
        outs = [(n_in, 2, m_in, STRIPE), (n_out, 2, m_out, STRIPE), w_in.shape, w_out.shape, row_in.shape, col_in.shape,
                (1, m_out), (cols_out // LANES, LANES), (8, LANES), (kinds, m_in, LANES), (m_out, LANES), (2, stripes * STRIPE // LANES, 1, LANES)]
        vmem = [((2 * m_in, tokens), jnp.bfloat16), ((2 * m_out, tokens), jnp.bfloat16), ((slots, tokens, STRIPE), jnp.bfloat16),
                ((n_in, m_in, STRIPE), F32), ((n_out, m_out, STRIPE), F32), ((1 + 2 * stripes, 2, LANES), F32),
                ((early // 2, n // 2, 4, 2, LANES), F32), ((single, n // 2, 2, 2, LANES), F32), ((n // 2, 2, LANES), F32), ((n, 2, 2, LANES), F32), ((2, 1 + 2 * stripes, 2, LANES), F32),
                ((kinds, 2 * m_in, LANES), F32), ((2 * m_out, LANES), F32), ((kinds, m_in, LANES), F32), ((m_out, LANES), F32), ((2, 2 * m_in, HALF), F32),
                ((1, LANES), F32), ((n, 1, LANES), F32),
                (row_in.shape, F32), (col_in.shape, F32), ((1, m_out), F32), ((cols_out // LANES, LANES), F32)]
        vmem.append(((8, LANES), F32))
        sems = [(2 * slots,), (2,), (2,), (5,), (2, 2), (2, 2), (2,), (2,), (2,), (2,), (2,), (2, 2), (2,)]
        anywhere = pl.BlockSpec(memory_space=pl.ANY)
        mid = pl.pallas_call(
            lambda *refs: grads_kernel(n, *refs),
            out_shape=[pltpu.VMEM(s, F32) for s in outs],
            in_specs=[anywhere] * len(ins),
            out_specs=[inside] * len(outs),
            scratch_shapes=[pltpu.VMEM(*v) for v in vmem] + [pltpu.SemaphoreType.DMA(s) for s in sems],
            compiler_params=pltpu.CompilerParams(collective_id=0, has_side_effects=True, vmem_limit_bytes=56 * 2**20),
            name='grads',
        )(*ins)
        finals = [w_in.shape, row_in.shape, col_in.shape, w_out.shape, (1, m_out), (cols_out // LANES, LANES)]
        new = pl.pallas_call(
            apply_kernel,
            out_shape=[jax.ShapeDtypeStruct(s, F32) for s in finals],
            in_specs=[inside] * len(mid),
            out_specs=[anywhere] * len(finals),
            scratch_shapes=[pltpu.VMEM(w_in.shape, F32), pltpu.VMEM(w_out.shape, F32), pltpu.SemaphoreType.DMA((2 * stripes + 4,))],
            compiler_params=pltpu.CompilerParams(vmem_limit_bytes=8 * 2**20),
            name='apply',
        )(*mid)
        return (new[0], new[1], new[2], new[3], new[4].reshape(m_out), new[5].reshape(cols_out))

    in_specs = (P(None, 'tp'), P(None, 'tp'), P(), P(), P(None, 'tp', None), P('tp', None),
                P(None, 'tp'), P(), P('tp'), P(), P(), P(), P(), P())
    out_specs = (P(None, 'tp', None), P(None, 'tp'), P(), P('tp', None), P('tp'), P())
    return jax.shard_map(local_step, mesh=mesh, in_specs=in_specs, out_specs=out_specs, check_vma=False)
```

```python
import jax
import jax.numpy as jnp
from jax import lax
from jax.experimental import pallas as pl
from jax.experimental.pallas import tpu as pltpu
from jax.sharding import PartitionSpec as P

EPS_ONE = 1e-30
EPS_TWO = 1e-3
LANES = 128
STRIPE = 512
HALF = STRIPE // 2
PARTS = 4
AHEAD = 6
F32 = jnp.float32
MESH = pl.DeviceIdType.MESH


def grads_kernel(n, x_hbm, h_hbm, dyi_hbm, dyo_hbm, wi_hbm, wo_hbm, ri_hbm, ci_hbm, ro_hbm, co_hbm,
                 scal_hbm,
                 gi, go, wi, wo, ri_new, ci_new, ro_new, co_new, coef, ai, ao, colf,
                 xs, hs, dy, si, so, csend, land, mid_land, misc_land, last_land, csum, ri_sq, ro_sq, ri_got, ro_got, split,
                 fsend, f_land, ri, ci, ro, co, scal,
                 dy_sem, w_sem, xs_sem, g_sem, land_sem, mid_sem, misc_sem, last_sem, fwd_sem, row_sem, f_sem):
    me = lax.axis_index('tp')
    core = lax.rem(me, 2)
    chip = me // 2
    x, y, z = lax.rem(chip, 2), lax.rem(chip // 2, 2), chip // 4
    partner = me + 1 - 2 * core
    high = z // 2
    planes = [3 * (1 - high), 2 - high, z + 1 - 2 * lax.rem(z, 2), z]
    same, everyone = [], []
    for plane in planes:
        for far_y in (1, 0):
            for far_x in (1, 0):
                for other in (0, 1):
                    if plane is z and not (far_y or far_x or other):
                        continue
                    place = (plane * 2 + lax.rem(y + far_y, 2)) * 2 + lax.rem(x + far_x, 2)
                    everyone.append(2 * place + lax.rem(core + other, 2))
                    if not other:
                        same.append(everyone[-1])
    kinds, m_in, cols_in = wi.shape
    m_out, cols_out = wo.shape
    half_in, half_out = cols_in // 2, cols_out // 2
    per_in, per_out = half_in // STRIPE, half_out // STRIPE
    n_in = kinds * per_in
    stripes = n_in + per_out
    slots, tokens = dy.shape[0:2]
    early = 2 * land.shape[0]
    single = mid_land.shape[0]
    shared = early + single

    def remote(src, dst, sems, peer):
        return pltpu.make_async_remote_copy(src_ref=src, dst_ref=dst, send_sem=sems.at[0], recv_sem=sems.at[1],
                                            device_id=(peer,), device_id_type=MESH)

    def to_all(src, dst, sems, who):
        for peer in who:
            remote(src, dst, sems, peer).start()

    def wait_for(ref, sem):
        pltpu.make_async_copy(ref, ref, sem).wait()

    def out_copy(s):
        cols = pl.ds(pl.multiple_of(core * half_out + s * STRIPE, LANES), STRIPE)
        return pltpu.make_async_copy(dyo_hbm.at[:, cols], dy.at[s], dy_sem.at[s + AHEAD // 2])

    def in_copy(t):
        slot = lax.rem(t + per_out, slots)
        cols = pl.ds(pl.multiple_of(core * half_in + lax.rem(t, per_in) * STRIPE, LANES), STRIPE)
        return pltpu.make_async_copy(dyi_hbm.at[t // per_in, :, cols], dy.at[slot], dy_sem.at[lax.rem(t, AHEAD)])

    def last_copy(part):
        t = n_in - 1
        slot = (t + per_out) % slots
        some = pl.ds(part * (tokens // PARTS), tokens // PARTS)
        cols = pl.ds(pl.multiple_of(core * half_in + t % per_in * STRIPE, LANES), STRIPE)
        return pltpu.make_async_copy(dyi_hbm.at[t // per_in, some, cols], dy.at[slot, some, :], dy_sem.at[(t + part) % AHEAD])

    barrier = pltpu.get_barrier_semaphore()
    x_copy = pltpu.make_async_copy(x_hbm, xs.at[pl.ds(0, m_in)], w_sem.at[0])
    h_copy = pltpu.make_async_copy(h_hbm, hs.at[pl.ds(0, m_out)], w_sem.at[1])
    x_copy.start()
    h_copy.start()
    out_copy(0).start()
    for peer in everyone:
        pl.semaphore_signal(barrier, inc=1, device_id=(peer,), device_id_type=MESH)
    for s in range(1, per_out):
        out_copy(s).start()
    small = [pltpu.make_async_copy(src, dst, sem.at[0]) for src, dst, sem in (
        (ri_hbm, ri, land_sem), (ci_hbm, ci, mid_sem), (ro_hbm, ro, misc_sem), (co_hbm, co, last_sem), (scal_hbm, scal, fwd_sem))]
    for copy in small:
        copy.start()

    def put_cols(p, h, col_sq, add):
        for r in range(2):
            part = col_sq[:, r * LANES:(r + 1) * LANES]
            where = (1 + 2 * p + h, pl.ds(r, 1), slice(None))
            csend[where] = csend[where] + part if add else part

    def share(pair):
        mine = csend.at[pl.ds(1 + 4 * pair, 4)]
        to_all(mine, land.at[pair, chip], land_sem, same)
        land[pair, chip] = mine[...]

    def add_rows(ref, where, sq):
        ref[where] = ref[where] + (sq[:, 0:LANES] + sq[:, LANES:HALF])

    ri_sq[...] = jnp.zeros_like(ri_sq)
    ro_sq[...] = jnp.zeros_like(ro_sq)
    x_copy.wait()
    h_copy.wait()
    in_copy(0).start()
    in_copy(1).start()
    in_copy(2).start()
    pl.semaphore_wait(barrier, n - 1)
    h_send = remote(hs.at[pl.ds(0, m_out)], hs.at[pl.ds(m_out, m_out)], xs_sem.at[1], partner)
    x_send = remote(xs.at[pl.ds(0, m_in)], xs.at[pl.ds(m_in, m_in)], xs_sem.at[0], partner)
    x_send.start()
    h_send.start()

    for s in range(per_out):
        out_copy(s).wait()
        in_copy(s + 3).start()
        for h in range(2):
            cols = pl.ds(h * HALF, HALF)
            own = jnp.dot(hs[0:m_out, :], dy[s, :, cols], preferred_element_type=F32)
            go[s, core, :, cols] = own
            own = own * own
            put_cols(s, h, jnp.sum(own, axis=0, keepdims=True), False)
            add_rows(ro_sq, (pl.ds(0, m_out), slice(None)), own)
    for copy in small:
        copy.wait()
    lane = lax.broadcasted_iota(jnp.int32, (1, LANES), 1)

    def pack(values):
        row = jnp.zeros((1, LANES), F32)
        for i, value in enumerate(values):
            row = jnp.where(lane == i, value, row)
        return row

    csend[0, 1:2, :] = jnp.zeros((1, LANES), F32)
    csend[0, 0:1, :] = pack([jnp.sum(ri[k:k + 1, :], axis=1, keepdims=True) for k in range(kinds)]
                            + [jnp.sum(ro[...], axis=1, keepdims=True)]) + scal[0:1, :]
    to_all(csend.at[0], misc_land.at[chip], misc_sem, same)
    misc_land[chip] = csend[0]
    x_send.wait_recv()
    in_copy(5).start()

    def partner_rows():
        h_send.wait_recv()
        for s in range(per_out):
            for h in range(2):
                cols = pl.ds(h * HALF, HALF)
                other = jnp.dot(hs[m_out:2 * m_out, :], dy[s, :, cols], preferred_element_type=F32)
                so[s, :, cols] = other
                other = other * other
                put_cols(s, h, jnp.sum(other, axis=0, keepdims=True), True)
                add_rows(ro_sq, (pl.ds(m_out, m_out), slice(None)), other)
        remote(so, go.at[:, core], g_sem.at[0], partner).start()
        remote(ro_sq.at[pl.ds(m_out, m_out)], ro_got, row_sem.at[0], partner).start()
        share(0)

    def product(t):
        p = t + per_out
        for h in range(2):
            cols = pl.ds(h * HALF, HALF)
            both = jnp.dot(xs[...], dy[lax.rem(p, slots), :, cols], preferred_element_type=F32)
            gi[t, core, :, cols] = both[0:m_in]
            si[t, :, cols] = both[m_in:2 * m_in]
            both = both * both
            put_cols(p, h, jnp.sum(both, axis=0, keepdims=True), False)
            add_rows(ri_sq, t // per_in, both)

    def give(t, size):
        remote(si.at[pl.ds(t, size)], gi.at[pl.ds(t, size), core], g_sem.at[1], partner).start()

    def in_step(i, carry):
        @pl.when(i == 1)
        def _():
            partner_rows()

        for t in (2 * i, 2 * i + 1):
            in_copy(t).wait()

            @pl.when(t + AHEAD < n_in - 1)
            def _():
                in_copy(t + AHEAD).start()

            for part in range(PARTS):
                @pl.when(t + AHEAD == n_in - 1 + part)
                def _():
                    last_copy(part).start()

        for t in (2 * i, 2 * i + 1):
            product(t)
        share(i + 1)
        give(2 * i, 2)
        return carry

    lax.fori_loop(0, early // 2 - 1, in_step, 0)
    def single_step(t, carry):
        in_copy(t).wait()
        for part in range(PARTS):
            @pl.when(t + AHEAD == n_in - 1 + part)
            def _():
                last_copy(part).start()

        product(t)
        p = t + per_out
        mine = csend.at[pl.ds(1 + 2 * p, 2)]
        to_all(mine, mid_land.at[p - early, chip], mid_sem, same)
        mid_land[p - early, chip] = mine[...]
        give(t, 1)
        return carry

    lax.fori_loop(early - per_out, n_in - 1, single_step, 0)
    t = n_in - 1
    for part in range(PARTS):
        some = pl.ds(part * (tokens // PARTS), tokens // PARTS)
        last_copy(part).wait()
        if part == PARTS - 1:
            wi_copy = pltpu.make_async_copy(wi_hbm, wi, w_sem.at[0])
            wo_copy = pltpu.make_async_copy(wo_hbm, wo, w_sem.at[1])
            wi_copy.start()
            wo_copy.start()
        for h in range(2):
            cols = pl.ds(h * HALF, HALF)
            both = jnp.dot(xs[:, some], dy[(t + per_out) % slots, some, cols], preferred_element_type=F32)
            if part:
                both = split[h] + both
            if part < PARTS - 1:
                split[h] = both
                continue
            gi[t, core, :, cols] = both[0:m_in]
            si[t, :, cols] = both[m_in:2 * m_in]
            both = both * both
            put_cols(t + per_out, h, jnp.sum(both, axis=0, keepdims=True), False)
            add_rows(ri_sq, t // per_in, both)
    mine = csend.at[pl.ds(1 + 2 * shared, 2)]
    to_all(mine, last_land.at[me], last_sem, everyone)
    last_land[me] = mine[...]
    remote(ri_sq.at[:, pl.ds(m_in, m_in)], ri_got, row_sem.at[1], partner).start()
    give(n_in - 1, 1)
    wait_for(misc_land.at[pl.ds(0, n // 2 - 1)], misc_sem.at[1])
    wait_for(land.at[:, pl.ds(0, n // 2 - 1)], land_sem.at[1])
    csum[core, 0] = jnp.sum(misc_land[...], axis=0)
    for pair in range(early // 2):
        csum[core, pl.ds(1 + 4 * pair, 4)] = jnp.sum(land[pair], axis=0)
    wait_for(mid_land.at[:, pl.ds(0, n // 2 - 1)], mid_sem.at[1])
    for i in range(single):
        csum[core, pl.ds(1 + 2 * (early + i), 2)] = jnp.sum(mid_land[i], axis=0)
    done = csum.at[core, pl.ds(0, 1 + 2 * shared)]
    forward = remote(done, done, fwd_sem, partner)
    forward.start()
    wait_for(ro_got, row_sem.at[0, 1])
    wait_for(ri_got, row_sem.at[1, 1])
    row_sums = [jnp.sum(ri_sq[k, 0:m_in] + ri_got[k], axis=1, keepdims=True) for k in range(kinds)]
    row_sums.append(jnp.sum(ro_sq[0:m_out] + ro_got[...], axis=1, keepdims=True))
    def square_sum(ref, cols):
        rows = ref.shape[0]
        total = [jnp.zeros((8, LANES), F32) for _ in range(4)]
        for r in range(cols // LANES):
            for b in range(rows // 8):
                w = ref[8 * b:8 * (b + 1), r * LANES:(r + 1) * LANES]
                total[b % 4] = total[b % 4] + w * w
        total = (total[0] + total[1]) + (total[2] + total[3])
        return jnp.sum(jnp.sum(total, axis=0, keepdims=True), axis=1, keepdims=True)

    wi_copy.wait()
    wo_copy.wait()
    w_sums = [square_sum(wi.at[k], cols_in) for k in range(kinds)] + [square_sum(wo, cols_out)]
    forward.wait_recv()
    first = [1 + 2 * (per_out + k * per_in) for k in range(kinds)] + [1]
    count = [2 * per_in] * kinds + [2 * per_out]
    rows_of = [m_in * n] * kinds + [m_out * n]
    cols_of = [cols_in] * kinds + [cols_out]

    def at_lane(row, i):
        return jnp.sum(jnp.where(lane == i, row, 0.0), axis=1, keepdims=True)

    misc = csum[0, 0, 0:1, :] + csum[1, 0, 0:1, :]
    keep, norm, step, rms = (at_lane(misc, kinds + 1 + i) for i in range(4))
    mix = 1.0 - keep
    eyes, olds, levels, grand = [], [], [], []
    for i in range(kinds + 1):
        rows = m_out if i == kinds else m_in
        eyes.append(lax.broadcasted_iota(jnp.int32, (rows, rows), 0) == lax.broadcasted_iota(jnp.int32, (rows, rows), 1))
        old = ro[...] if i == kinds else ri[i:i + 1, :]
        olds.append(keep * jnp.sum(jnp.where(eyes[i], old, 0.0), axis=1, keepdims=True))
        levels.append(keep * (at_lane(misc, i) / rows_of[i]))
        known = min(first[i] + count[i], 1 + 2 * shared)
        grand.append(jnp.sum(csum[:, first[i]:known], axis=(0, 1)))
    wait_for(last_land.at[pl.ds(0, n - 1)], last_sem.at[1])
    for c in range(2):
        total = last_land[c]
        for q in range(1, n // 2):
            total = total + last_land[2 * q + c]
        csum[c, pl.ds(1 + 2 * shared, 2)] = total
        grand[kinds - 1] = grand[kinds - 1] + jnp.sum(total, axis=0)
    grand = [jnp.sum(jnp.sum(g, axis=0, keepdims=True), axis=1, keepdims=True) for g in grand]
    norm_sq = grand[0]
    for g in grand[1:]:
        norm_sq = norm_sq + g
    scale = jnp.minimum(1.0, norm / jnp.sqrt(norm_sq))

    for i in range(kinds + 1):
        rows = m_out if i == kinds else m_in
        level = levels[i] + mix * (scale * (scale * (grand[i] / (rows_of[i] * cols_of[i]))) + EPS_ONE)
        new = olds[i] + mix * (scale * (scale * (row_sums[i] / cols_of[i])) + EPS_ONE)
        factor = jnp.broadcast_to(scale * lax.rsqrt(new / level), (rows, LANES))
        if i == kinds:
            ao[...] = factor
        else:
            ai[i] = factor
        olds[i] = new

    for c in range(2):
        for p in range(stripes):
            for r in range(STRIPE // LANES):
                where = (c, 1 + 2 * p + r // 2, pl.ds(r % 2, 1), slice(None))
                if p < per_out:
                    i = kinds
                    spot = (pl.ds((c * half_out + p * STRIPE) // LANES + r, 1), slice(None))
                    old, store = co, co_new
                else:
                    i, s = divmod(p - per_out, per_in)
                    spot = (pl.ds(i, 1), pl.ds(c * half_in + s * STRIPE + r * LANES, LANES))
                    old, store = ci, ci_new
                new = keep * old[spot] + mix * (scale * (scale * (csum[where] / rows_of[i])) + EPS_ONE)
                store[spot] = new
                colf[c, STRIPE // LANES * p + r] = lax.rsqrt(new)

    wait_for(so, g_sem.at[0, 1])
    wait_for(si, g_sem.at[1, 1])
    def update_sq(ref, factor, p0, blocks):
        rows = ref.shape[2]

        def add(t, total):
            for c in range(2):
                for r in range(STRIPE // LANES):
                    part = ref[t, c, :, r * LANES:(r + 1) * LANES] * factor
                    part = part * part
                    fold = part[0:8]
                    for b in range(1, rows // 8):
                        fold = fold + part[8 * b:8 * (b + 1)]
                    col = colf[c, STRIPE // LANES * (p0 + t) + r]
                    total = total + fold * (col * col)
            return total

        total = lax.fori_loop(blocks[0], blocks[1], add, jnp.zeros((8, LANES), F32), unroll=True)
        return jnp.sum(jnp.sum(total, axis=0, keepdims=True), axis=1, keepdims=True)

    u_sums = [update_sq(gi, ai[k], per_out, (k * per_in, (k + 1) * per_in)) for k in range(kinds)]
    u_sums.append(update_sq(go, ao[...], 0, (0, per_out)))
    fsend[...] = pack(u_sums + w_sums)
    to_all(fsend, f_land.at[me], f_sem, everyone)
    f_land[me] = fsend[...]

    for i in range(kinds + 1):
        flat = jnp.sum(jnp.where(eyes[i], olds[i], 0.0), axis=0, keepdims=True)
        if i == kinds:
            ro_new[...] = flat
        else:
            ri_new[i:i + 1, :] = flat

    x_send.wait_send()
    h_send.wait_send()
    forward.wait_send()
    wait_for(so, g_sem.at[0, 0])
    wait_for(si, g_sem.at[1, 0])
    wait_for(misc_land.at[pl.ds(0, n // 2 - 1)], misc_sem.at[0])
    wait_for(land.at[:, pl.ds(0, n // 2 - 1)], land_sem.at[0])
    wait_for(mid_land.at[:, pl.ds(0, n // 2 - 1)], mid_sem.at[0])
    wait_for(ro_got, row_sem.at[0, 0])
    wait_for(ri_got, row_sem.at[1, 0])
    wait_for(last_land.at[pl.ds(0, n - 1)], last_sem.at[0])
    wait_for(f_land.at[pl.ds(0, n - 1)], f_sem.at[1])
    sums = f_land[0]
    for d in range(1, n):
        sums = sums + f_land[d]
    for i in range(kinds + 1):
        size = float(rows_of[i] * cols_of[i])
        clip = jnp.maximum(1.0, jnp.sqrt(at_lane(sums, i) / size) / rms)
        move = step * jnp.maximum(EPS_TWO, jnp.sqrt(at_lane(sums, kinds + 1 + i) / size))
        coef[i:i + 1, :] = jnp.broadcast_to(move / clip, (1, LANES))
    wait_for(f_land.at[pl.ds(0, n - 1)], f_sem.at[0])


def scalar_kernel(place, one, two, row):
    lane = lax.broadcasted_iota(jnp.int32, (8, LANES), 1)
    row[...] = jnp.where(lane == place, one[...], jnp.where(lane == place + 1, two[...], 0.0))


def apply_kernel(gi, go, wi, wo, ri, ci, ro, co, coef, ai, ao, colf, wi_out, ri_out, ci_out, wo_out, ro_out, co_out, wi_new, wo_new, sems):
    kinds, m_in, cols_in = wi.shape
    per_in, per_out = gi.shape[0] // kinds, go.shape[0]
    lanes = STRIPE // LANES

    def send(src, dst, sem):
        copy = pltpu.make_async_copy(src, dst, sems.at[sem])
        copy.start()
        return copy

    def blocks(factor, g, p, c, old, new, out, first, sem):
        for r in range(lanes):
            cols = pl.ds(first + r * LANES, LANES)
            new[:, cols] = old[:, cols] - (factor * colf[c, lanes * p + r]) * g[:, r * LANES:(r + 1) * LANES]
        part = pl.ds(first, STRIPE)
        send(new.at[:, part], out.at[:, part], sem)

    for c in range(2):
        factor = ao[...] * coef[kinds:kinds + 1, :]
        for s in range(per_out):
            blocks(factor, go.at[s, c], s, c, wo, wo_new, wo_out, c * (wo.shape[1] // 2) + s * STRIPE, 0)
    small = [send(src, dst, 2 + i) for i, (src, dst) in enumerate(((ri, ri_out), (ci, ci_out), (ro, ro_out), (co, co_out)))]
    for k in range(kinds):
        factor = ai[k] * coef[k:k + 1, :]
        for c in range(2):
            for s in range(per_in):
                t = k * per_in + s
                blocks(factor, gi.at[t, c], per_out + t, c, wi.at[k], wi_new.at[k], wi_out.at[k], c * (cols_in // 2) + s * STRIPE, 1)
    for copy in small:
        copy.wait()
    pltpu.make_async_copy(wo_new, wo_out, sems.at[0]).wait()
    pltpu.make_async_copy(wi_new, wi_out, sems.at[1]).wait()


def solution(mesh):
    n = mesh.shape['tp']

    def local_step(x_norm, hid_act, dy_in, dy_out, w_in, w_out, row_in, col_in, row_out, col_out, beta_two, rel_step, clip_rms, clip_norm):
        kinds, m_in, cols_in = w_in.shape
        m_out, cols_out = w_out.shape
        tokens = x_norm.shape[0]
        inside = pl.BlockSpec(memory_space=pltpu.VMEM)
        scalars = lax.switch(
            jnp.minimum(lax.axis_index('tp'), 2),
            [lambda *values, i=i: pl.pallas_call(
                lambda *refs: scalar_kernel(kinds + 1 + 2 * i, *refs), out_shape=jax.ShapeDtypeStruct((8, LANES), F32),
                in_specs=[inside] * 2, out_specs=inside, name='scalar')(*[v.reshape(1, 1) for v in values[2 * i:2 * i + 2]]) for i in range(2)]
            + [lambda *values: jnp.zeros((8, LANES), F32)],
            beta_two, clip_norm, rel_step, clip_rms)
        n_in, n_out = kinds * cols_in // (2 * STRIPE), cols_out // (2 * STRIPE)
        stripes = n_in + n_out
        single = 3
        early = stripes - single - 1
        slots = 10
        ins = [x_norm.T, hid_act.T, dy_in, dy_out, w_in, w_out, row_in, col_in, row_out.reshape(1, -1), col_out.reshape(-1, LANES)]
        ins.append(scalars)
        outs = [(n_in, 2, m_in, STRIPE), (n_out, 2, m_out, STRIPE), w_in.shape, w_out.shape, row_in.shape, col_in.shape,
                (1, m_out), (cols_out // LANES, LANES), (8, LANES), (kinds, m_in, LANES), (m_out, LANES), (2, stripes * STRIPE // LANES, 1, LANES)]
        vmem = [((2 * m_in, tokens), jnp.bfloat16), ((2 * m_out, tokens), jnp.bfloat16), ((slots, tokens, STRIPE), jnp.bfloat16),
                ((n_in, m_in, STRIPE), F32), ((n_out, m_out, STRIPE), F32), ((1 + 2 * stripes, 2, LANES), F32),
                ((early // 2, n // 2, 4, 2, LANES), F32), ((single, n // 2, 2, 2, LANES), F32), ((n // 2, 2, LANES), F32), ((n, 2, 2, LANES), F32), ((2, 1 + 2 * stripes, 2, LANES), F32),
                ((kinds, 2 * m_in, LANES), F32), ((2 * m_out, LANES), F32), ((kinds, m_in, LANES), F32), ((m_out, LANES), F32), ((2, 2 * m_in, HALF), F32),
                ((1, LANES), F32), ((n, 1, LANES), F32),
                (row_in.shape, F32), (col_in.shape, F32), ((1, m_out), F32), ((cols_out // LANES, LANES), F32)]
        vmem.append(((8, LANES), F32))
        sems = [(AHEAD,), (2,), (2, 2), (2, 2), (2,), (2,), (2,), (2,), (2,), (2, 2), (2,)]
        anywhere = pl.BlockSpec(memory_space=pl.ANY)
        mid = pl.pallas_call(
            lambda *refs: grads_kernel(n, *refs),
            out_shape=[pltpu.VMEM(s, F32) for s in outs],
            in_specs=[anywhere] * len(ins),
            out_specs=[inside] * len(outs),
            scratch_shapes=[pltpu.VMEM(*v) for v in vmem] + [pltpu.SemaphoreType.DMA(s) for s in sems],
            compiler_params=pltpu.CompilerParams(collective_id=0, has_side_effects=True, vmem_limit_bytes=56 * 2**20),
            name='grads',
        )(*ins)
        finals = [w_in.shape, row_in.shape, col_in.shape, w_out.shape, (1, m_out), (cols_out // LANES, LANES)]
        new = pl.pallas_call(
            apply_kernel,
            out_shape=[jax.ShapeDtypeStruct(s, F32) for s in finals],
            in_specs=[inside] * len(mid),
            out_specs=[anywhere] * len(finals),
            scratch_shapes=[pltpu.VMEM(w_in.shape, F32), pltpu.VMEM(w_out.shape, F32), pltpu.SemaphoreType.DMA((6,))],
            compiler_params=pltpu.CompilerParams(vmem_limit_bytes=8 * 2**20),
            name='apply',
        )(*mid)
        return (new[0], new[1], new[2], new[3], new[4].reshape(m_out), new[5].reshape(cols_out))

    in_specs = (P(None, 'tp'), P(None, 'tp'), P(), P(), P(None, 'tp', None), P('tp', None),
                P(None, 'tp'), P(), P('tp'), P(), P(), P(), P(), P())
    out_specs = (P(None, 'tp', None), P(None, 'tp'), P(), P('tp', None), P('tp'), P())
    return jax.shard_map(local_step, mesh=mesh, in_specs=in_specs, out_specs=out_specs, check_vma=False)
```

```python
import jax
import jax.numpy as jnp
from jax import lax
from jax.experimental import pallas as pl
from jax.experimental.pallas import tpu as pltpu
from jax.sharding import PartitionSpec as P

EPS_ONE = 1e-30
EPS_TWO = 1e-3
LANES = 128
STRIPE = 512
HALF = STRIPE // 2
PARTS = 4
AHEAD = 6
F32 = jnp.float32
MESH = pl.DeviceIdType.MESH


def grads_kernel(n, x_hbm, h_hbm, dyi_hbm, dyo_hbm, wi_hbm, wo_hbm, ri_hbm, ci_hbm, ro_hbm, co_hbm,
                 scal_hbm,
                 gi, go, wi, wo, ri_new, ci_new, ro_new, co_new, coef, ai, ao, colf,
                 xs, hs, dy, si, so, csend, land, mid_land, misc_land, last_land, csum, ri_sq, ro_sq, ri_got, ro_got, split,
                 fsend, f_land, ri, ci, ro, co, scal,
                 dy_sem, w_sem, xs_sem, g_sem, land_sem, mid_sem, misc_sem, last_sem, fwd_sem, row_sem, f_sem):
    me = lax.axis_index('tp')
    core = lax.rem(me, 2)
    chip = me // 2
    x, y, z = lax.rem(chip, 2), lax.rem(chip // 2, 2), chip // 4
    partner = me + 1 - 2 * core
    high = z // 2
    planes = [3 * (1 - high), 2 - high, z + 1 - 2 * lax.rem(z, 2), z]
    same, everyone = [], []
    for plane in planes:
        for far_y in (1, 0):
            for far_x in (1, 0):
                for other in (0, 1):
                    if plane is z and not (far_y or far_x or other):
                        continue
                    place = (plane * 2 + lax.rem(y + far_y, 2)) * 2 + lax.rem(x + far_x, 2)
                    everyone.append(2 * place + lax.rem(core + other, 2))
                    if not other:
                        same.append(everyone[-1])
    kinds, m_in, cols_in = wi.shape
    m_out, cols_out = wo.shape
    half_in, half_out = cols_in // 2, cols_out // 2
    per_in, per_out = half_in // STRIPE, half_out // STRIPE
    n_in = kinds * per_in
    stripes = n_in + per_out
    slots, tokens = dy.shape[0:2]
    early = 2 * land.shape[0]
    single = mid_land.shape[0]
    shared = early + single

    def remote(src, dst, sems, peer):
        return pltpu.make_async_remote_copy(src_ref=src, dst_ref=dst, send_sem=sems.at[0], recv_sem=sems.at[1],
                                            device_id=(peer,), device_id_type=MESH)

    def to_all(src, dst, sems, who):
        for peer in who:
            remote(src, dst, sems, peer).start()

    def wait_for(ref, sem):
        pltpu.make_async_copy(ref, ref, sem).wait()

    def out_copy(s):
        cols = pl.ds(pl.multiple_of(core * half_out + s * STRIPE, LANES), STRIPE)
        return pltpu.make_async_copy(dyo_hbm.at[:, cols], dy.at[s], dy_sem.at[s + AHEAD // 2])

    def in_copy(t):
        slot = lax.rem(t + per_out, slots)
        cols = pl.ds(pl.multiple_of(core * half_in + lax.rem(t, per_in) * STRIPE, LANES), STRIPE)
        return pltpu.make_async_copy(dyi_hbm.at[t // per_in, :, cols], dy.at[slot], dy_sem.at[lax.rem(t, AHEAD)])

    def last_copy(part):
        t = n_in - 1
        slot = (t + per_out) % slots
        some = pl.ds(part * (tokens // PARTS), tokens // PARTS)
        cols = pl.ds(pl.multiple_of(core * half_in + t % per_in * STRIPE, LANES), STRIPE)
        return pltpu.make_async_copy(dyi_hbm.at[t // per_in, some, cols], dy.at[slot, some, :], dy_sem.at[(t + part) % AHEAD])

    barrier = pltpu.get_barrier_semaphore()
    x_copy = pltpu.make_async_copy(x_hbm, xs.at[pl.ds(0, m_in)], w_sem.at[0])
    h_copy = pltpu.make_async_copy(h_hbm, hs.at[pl.ds(0, m_out)], w_sem.at[1])
    x_copy.start()
    h_copy.start()
    out_copy(0).start()
    for peer in everyone:
        pl.semaphore_signal(barrier, inc=1, device_id=(peer,), device_id_type=MESH)
    for s in range(1, per_out):
        out_copy(s).start()
    small = [pltpu.make_async_copy(src, dst, sem.at[0]) for src, dst, sem in (
        (ri_hbm, ri, land_sem), (ci_hbm, ci, mid_sem), (ro_hbm, ro, misc_sem), (co_hbm, co, last_sem), (scal_hbm, scal, fwd_sem))]
    for copy in small:
        copy.start()

    def put_cols(p, h, col_sq, add):
        for r in range(2):
            part = col_sq[:, r * LANES:(r + 1) * LANES]
            where = (1 + 2 * p + h, pl.ds(r, 1), slice(None))
            csend[where] = csend[where] + part if add else part

    def share(pair):
        mine = csend.at[pl.ds(1 + 4 * pair, 4)]
        to_all(mine, land.at[pair, chip], land_sem, same)
        land[pair, chip] = mine[...]

    def add_rows(ref, where, sq):
        ref[where] = ref[where] + (sq[:, 0:LANES] + sq[:, LANES:HALF])

    ri_sq[...] = jnp.zeros_like(ri_sq)
    ro_sq[...] = jnp.zeros_like(ro_sq)
    x_copy.wait()
    h_copy.wait()
    in_copy(0).start()
    in_copy(1).start()
    in_copy(2).start()
    pl.semaphore_wait(barrier, n - 1)
    h_send = remote(hs.at[pl.ds(0, m_out)], hs.at[pl.ds(m_out, m_out)], xs_sem.at[1], partner)
    x_send = remote(xs.at[pl.ds(0, m_in)], xs.at[pl.ds(m_in, m_in)], xs_sem.at[0], partner)
    x_send.start()
    h_send.start()

    for s in range(per_out):
        out_copy(s).wait()
        in_copy(s + 3).start()
        for h in range(2):
            cols = pl.ds(h * HALF, HALF)
            own = jnp.dot(hs[0:m_out, :], dy[s, :, cols], preferred_element_type=F32)
            go[s, core, :, cols] = own
            own = own * own
            put_cols(s, h, jnp.sum(own, axis=0, keepdims=True), False)
            add_rows(ro_sq, (pl.ds(0, m_out), slice(None)), own)
    for copy in small:
        copy.wait()
    lane = lax.broadcasted_iota(jnp.int32, (1, LANES), 1)

    def pack(values):
        row = jnp.zeros((1, LANES), F32)
        for i, value in enumerate(values):
            row = jnp.where(lane == i, value, row)
        return row

    csend[0, 1:2, :] = jnp.zeros((1, LANES), F32)
    csend[0, 0:1, :] = pack([jnp.sum(ri[k:k + 1, :], axis=1, keepdims=True) for k in range(kinds)]
                            + [jnp.sum(ro[...], axis=1, keepdims=True)]) + scal[0:1, :]
    to_all(csend.at[0], misc_land.at[chip], misc_sem, same)
    misc_land[chip] = csend[0]
    x_send.wait_recv()
    in_copy(5).start()

    def partner_rows():
        h_send.wait_recv()
        for s in range(per_out):
            for h in range(2):
                cols = pl.ds(h * HALF, HALF)
                other = jnp.dot(hs[m_out:2 * m_out, :], dy[s, :, cols], preferred_element_type=F32)
                so[s, :, cols] = other
                other = other * other
                put_cols(s, h, jnp.sum(other, axis=0, keepdims=True), True)
                add_rows(ro_sq, (pl.ds(m_out, m_out), slice(None)), other)
        remote(so, go.at[:, core], g_sem.at[0], partner).start()
        remote(ro_sq.at[pl.ds(m_out, m_out)], ro_got, row_sem.at[0], partner).start()
        share(0)

    def product(t):
        p = t + per_out
        for h in range(2):
            cols = pl.ds(h * HALF, HALF)
            both = jnp.dot(xs[...], dy[lax.rem(p, slots), :, cols], preferred_element_type=F32)
            gi[t, core, :, cols] = both[0:m_in]
            si[t, :, cols] = both[m_in:2 * m_in]
            both = both * both
            put_cols(p, h, jnp.sum(both, axis=0, keepdims=True), False)
            add_rows(ri_sq, t // per_in, both)

    def give(t, size):
        remote(si.at[pl.ds(t, size)], gi.at[pl.ds(t, size), core], g_sem.at[1], partner).start()

    def in_step(i, carry):
        @pl.when(i == 1)
        def _():
            partner_rows()

        for t in (2 * i, 2 * i + 1):
            in_copy(t).wait()

            @pl.when(t + AHEAD < n_in - 1)
            def _():
                in_copy(t + AHEAD).start()

            for part in range(PARTS):
                @pl.when(t + AHEAD == n_in - 1 + part)
                def _():
                    last_copy(part).start()

        for t in (2 * i, 2 * i + 1):
            product(t)
        share(i + 1)
        give(2 * i, 2)
        return carry

    lax.fori_loop(0, early // 2 - 1, in_step, 0)
    def single_step(t, carry):
        in_copy(t).wait()
        for part in range(PARTS):
            @pl.when(t + AHEAD == n_in - 1 + part)
            def _():
                last_copy(part).start()

        product(t)
        p = t + per_out
        mine = csend.at[pl.ds(1 + 2 * p, 2)]
        to_all(mine, mid_land.at[p - early, chip], mid_sem, same)
        mid_land[p - early, chip] = mine[...]
        give(t, 1)
        return carry

    lax.fori_loop(early - per_out, n_in - 1, single_step, 0)
    t = n_in - 1
    for part in range(PARTS):
        some = pl.ds(part * (tokens // PARTS), tokens // PARTS)
        last_copy(part).wait()
        if part == PARTS - 1:
            wi_copy = pltpu.make_async_copy(wi_hbm, wi, w_sem.at[0])
            wo_copy = pltpu.make_async_copy(wo_hbm, wo, w_sem.at[1])
            wi_copy.start()
            wo_copy.start()
        for h in range(2):
            cols = pl.ds(h * HALF, HALF)
            both = jnp.dot(xs[:, some], dy[(t + per_out) % slots, some, cols], preferred_element_type=F32)
            if part:
                both = split[h] + both
            if part < PARTS - 1:
                split[h] = both
                continue
            gi[t, core, :, cols] = both[0:m_in]
            si[t, :, cols] = both[m_in:2 * m_in]
            both = both * both
            put_cols(t + per_out, h, jnp.sum(both, axis=0, keepdims=True), False)
            add_rows(ri_sq, t // per_in, both)
    mine = csend.at[pl.ds(1 + 2 * shared, 2)]
    to_all(mine, last_land.at[me], last_sem, everyone)
    last_land[me] = mine[...]
    remote(ri_sq.at[:, pl.ds(m_in, m_in)], ri_got, row_sem.at[1], partner).start()
    give(n_in - 1, 1)
    wait_for(misc_land.at[pl.ds(0, n // 2 - 1)], misc_sem.at[1])
    wait_for(land.at[:, pl.ds(0, n // 2 - 1)], land_sem.at[1])
    csum[core, 0] = jnp.sum(misc_land[...], axis=0)
    for pair in range(early // 2):
        csum[core, pl.ds(1 + 4 * pair, 4)] = jnp.sum(land[pair], axis=0)
    wait_for(mid_land.at[:, pl.ds(0, n // 2 - 1)], mid_sem.at[1])
    for i in range(single):
        csum[core, pl.ds(1 + 2 * (early + i), 2)] = jnp.sum(mid_land[i], axis=0)
    done = csum.at[core, pl.ds(0, 1 + 2 * shared)]
    forward = remote(done, done, fwd_sem, partner)
    forward.start()
    wait_for(ro_got, row_sem.at[0, 1])
    wait_for(ri_got, row_sem.at[1, 1])
    row_sums = [jnp.sum(ri_sq[k, 0:m_in] + ri_got[k], axis=1, keepdims=True) for k in range(kinds)]
    row_sums.append(jnp.sum(ro_sq[0:m_out] + ro_got[...], axis=1, keepdims=True))
    def square_sum(ref, cols):
        rows = ref.shape[0]
        total = [jnp.zeros((8, LANES), F32) for _ in range(4)]
        for r in range(cols // LANES):
            for b in range(rows // 8):
                w = ref[8 * b:8 * (b + 1), r * LANES:(r + 1) * LANES]
                total[b % 4] = total[b % 4] + w * w
        total = (total[0] + total[1]) + (total[2] + total[3])
        return jnp.sum(jnp.sum(total, axis=0, keepdims=True), axis=1, keepdims=True)

    wi_copy.wait()
    wo_copy.wait()
    w_sums = [square_sum(wi.at[k], cols_in) for k in range(kinds)] + [square_sum(wo, cols_out)]
    forward.wait_recv()
    first = [1 + 2 * (per_out + k * per_in) for k in range(kinds)] + [1]
    count = [2 * per_in] * kinds + [2 * per_out]
    rows_of = [m_in * n] * kinds + [m_out * n]
    cols_of = [cols_in] * kinds + [cols_out]

    def at_lane(row, i):
        return jnp.sum(jnp.where(lane == i, row, 0.0), axis=1, keepdims=True)

    misc = csum[0, 0, 0:1, :] + csum[1, 0, 0:1, :]
    keep, norm, step, rms = (at_lane(misc, kinds + 1 + i) for i in range(4))
    mix = 1.0 - keep
    eyes, olds, levels, grand = [], [], [], []
    for i in range(kinds + 1):
        rows = m_out if i == kinds else m_in
        eyes.append(lax.broadcasted_iota(jnp.int32, (rows, rows), 0) == lax.broadcasted_iota(jnp.int32, (rows, rows), 1))
        old = ro[...] if i == kinds else ri[i:i + 1, :]
        olds.append(keep * jnp.sum(jnp.where(eyes[i], old, 0.0), axis=1, keepdims=True))
        levels.append(keep * (at_lane(misc, i) / rows_of[i]))
        known = min(first[i] + count[i], 1 + 2 * shared)
        grand.append(jnp.sum(csum[:, first[i]:known], axis=(0, 1)))
    wait_for(last_land.at[pl.ds(0, n - 1)], last_sem.at[1])
    for c in range(2):
        total = last_land[c]
        for q in range(1, n // 2):
            total = total + last_land[2 * q + c]
        csum[c, pl.ds(1 + 2 * shared, 2)] = total
        grand[kinds - 1] = grand[kinds - 1] + jnp.sum(total, axis=0)
    grand = [jnp.sum(jnp.sum(g, axis=0, keepdims=True), axis=1, keepdims=True) for g in grand]
    norm_sq = grand[0]
    for g in grand[1:]:
        norm_sq = norm_sq + g
    scale = jnp.minimum(1.0, norm / jnp.sqrt(norm_sq))

    for i in range(kinds + 1):
        rows = m_out if i == kinds else m_in
        level = levels[i] + mix * (scale * (scale * (grand[i] / (rows_of[i] * cols_of[i]))) + EPS_ONE)
        new = olds[i] + mix * (scale * (scale * (row_sums[i] / cols_of[i])) + EPS_ONE)
        factor = jnp.broadcast_to(scale * lax.rsqrt(new / level), (rows, LANES))
        if i == kinds:
            ao[...] = factor
        else:
            ai[i] = factor
        olds[i] = new

    for c in range(2):
        for p in range(stripes):
            for r in range(STRIPE // LANES):
                where = (c, 1 + 2 * p + r // 2, pl.ds(r % 2, 1), slice(None))
                if p < per_out:
                    i = kinds
                    spot = (pl.ds((c * half_out + p * STRIPE) // LANES + r, 1), slice(None))
                    old, store = co, co_new
                else:
                    i, s = divmod(p - per_out, per_in)
                    spot = (pl.ds(i, 1), pl.ds(c * half_in + s * STRIPE + r * LANES, LANES))
                    old, store = ci, ci_new
                new = keep * old[spot] + mix * (scale * (scale * (csum[where] / rows_of[i])) + EPS_ONE)
                store[spot] = new
                colf[c, STRIPE // LANES * p + r] = lax.rsqrt(new)

    wait_for(so, g_sem.at[0, 1])
    wait_for(si, g_sem.at[1, 1])
    def update_sq(ref, factor, p0, blocks):
        rows = ref.shape[2]
        spots = [(t, c, r) for t in range(*blocks) for c in range(2) for r in range(STRIPE // LANES)]
        totals = [None] * len(spots)
        for b in range(rows // 8):
            some = slice(8 * b, 8 * (b + 1))
            weight = factor[some, :]
            for i, (t, c, r) in enumerate(spots):
                part = ref[t, c, some, r * LANES:(r + 1) * LANES] * weight
                part = part * part
                totals[i] = part if totals[i] is None else totals[i] + part
        parts = []
        for (t, c, r), total in zip(spots, totals):
            col = colf[c, STRIPE // LANES * (p0 + t) + r]
            parts.append(total * (col * col))
        while len(parts) > 1:
            parts = [a + b for a, b in zip(parts[::2], parts[1::2])] + parts[len(parts) // 2 * 2:]
        return jnp.sum(jnp.sum(parts[0], axis=0, keepdims=True), axis=1, keepdims=True)

    u_sums = [update_sq(gi, ai.at[k], per_out, (k * per_in, (k + 1) * per_in)) for k in range(kinds)]
    u_sums.append(update_sq(go, ao, 0, (0, per_out)))
    fsend[...] = pack(u_sums + w_sums)
    to_all(fsend, f_land.at[me], f_sem, everyone)
    f_land[me] = fsend[...]

    for i in range(kinds + 1):
        flat = jnp.sum(jnp.where(eyes[i], olds[i], 0.0), axis=0, keepdims=True)
        if i == kinds:
            ro_new[...] = flat
        else:
            ri_new[i:i + 1, :] = flat

    x_send.wait_send()
    h_send.wait_send()
    forward.wait_send()
    wait_for(so, g_sem.at[0, 0])
    wait_for(si, g_sem.at[1, 0])
    wait_for(misc_land.at[pl.ds(0, n // 2 - 1)], misc_sem.at[0])
    wait_for(land.at[:, pl.ds(0, n // 2 - 1)], land_sem.at[0])
    wait_for(mid_land.at[:, pl.ds(0, n // 2 - 1)], mid_sem.at[0])
    wait_for(ro_got, row_sem.at[0, 0])
    wait_for(ri_got, row_sem.at[1, 0])
    wait_for(last_land.at[pl.ds(0, n - 1)], last_sem.at[0])
    wait_for(f_land.at[pl.ds(0, n - 1)], f_sem.at[1])
    parts = [f_land[d] for d in range(n)]
    while len(parts) > 1:
        parts = [a + b for a, b in zip(parts[::2], parts[1::2])]
    sums = parts[0]
    for i in range(kinds + 1):
        size = float(rows_of[i] * cols_of[i])
        clip = jnp.maximum(1.0, jnp.sqrt(at_lane(sums, i) / size) / rms)
        move = step * jnp.maximum(EPS_TWO, jnp.sqrt(at_lane(sums, kinds + 1 + i) / size))
        coef[i:i + 1, :] = jnp.broadcast_to(move / clip, (1, LANES))
    wait_for(f_land.at[pl.ds(0, n - 1)], f_sem.at[0])


def scalar_kernel(place, one, two, row):
    lane = lax.broadcasted_iota(jnp.int32, (8, LANES), 1)
    row[...] = jnp.where(lane == place, one[...], jnp.where(lane == place + 1, two[...], 0.0))


def apply_kernel(gi, go, wi, wo, ri, ci, ro, co, coef, ai, ao, colf, wi_out, ri_out, ci_out, wo_out, ro_out, co_out, wi_new, wo_new, sems):
    kinds, m_in, cols_in = wi.shape
    per_in, per_out = gi.shape[0] // kinds, go.shape[0]
    lanes = STRIPE // LANES

    def send(src, dst, sem):
        copy = pltpu.make_async_copy(src, dst, sems.at[sem])
        copy.start()
        return copy

    def blocks(factor, g, p, c, old, new, out, first, sem):
        for r in range(lanes):
            cols = pl.ds(first + r * LANES, LANES)
            new[:, cols] = old[:, cols] - (factor * colf[c, lanes * p + r]) * g[:, r * LANES:(r + 1) * LANES]
        part = pl.ds(first, STRIPE)
        send(new.at[:, part], out.at[:, part], sem)

    small = [send(src, dst, 2 + i) for i, (src, dst) in enumerate(((ri, ri_out), (ci, ci_out), (ro, ro_out), (co, co_out)))]
    for c in range(2):
        factor = ao[...] * coef[kinds:kinds + 1, :]
        for s in range(per_out):
            blocks(factor, go.at[s, c], s, c, wo, wo_new, wo_out, c * (wo.shape[1] // 2) + s * STRIPE, 0)
    for k in range(kinds):
        factor = ai[k] * coef[k:k + 1, :]
        for c in range(2):
            for s in range(per_in):
                t = k * per_in + s
                blocks(factor, gi.at[t, c], per_out + t, c, wi.at[k], wi_new.at[k], wi_out.at[k], c * (cols_in // 2) + s * STRIPE, 1)
    for copy in small:
        copy.wait()
    pltpu.make_async_copy(wo_new, wo_out, sems.at[0]).wait()
    pltpu.make_async_copy(wi_new, wi_out, sems.at[1]).wait()


def solution(mesh):
    n = mesh.shape['tp']

    def local_step(x_norm, hid_act, dy_in, dy_out, w_in, w_out, row_in, col_in, row_out, col_out, beta_two, rel_step, clip_rms, clip_norm):
        kinds, m_in, cols_in = w_in.shape
        m_out, cols_out = w_out.shape
        tokens = x_norm.shape[0]
        inside = pl.BlockSpec(memory_space=pltpu.VMEM)
        scalars = lax.switch(
            jnp.minimum(lax.axis_index('tp'), 2),
            [lambda *values, i=i: pl.pallas_call(
                lambda *refs: scalar_kernel(kinds + 1 + 2 * i, *refs), out_shape=jax.ShapeDtypeStruct((8, LANES), F32),
                in_specs=[inside] * 2, out_specs=inside, name='scalar')(*[v.reshape(1, 1) for v in values[2 * i:2 * i + 2]]) for i in range(2)]
            + [lambda *values: jnp.zeros((8, LANES), F32)],
            beta_two, clip_norm, rel_step, clip_rms)
        n_in, n_out = kinds * cols_in // (2 * STRIPE), cols_out // (2 * STRIPE)
        stripes = n_in + n_out
        single = 3
        early = stripes - single - 1
        slots = 10
        ins = [x_norm.T, hid_act.T, dy_in, dy_out, w_in, w_out, row_in, col_in, row_out.reshape(1, -1), col_out.reshape(-1, LANES)]
        ins.append(scalars)
        outs = [(n_in, 2, m_in, STRIPE), (n_out, 2, m_out, STRIPE), w_in.shape, w_out.shape, row_in.shape, col_in.shape,
                (1, m_out), (cols_out // LANES, LANES), (8, LANES), (kinds, m_in, LANES), (m_out, LANES), (2, stripes * STRIPE // LANES, 1, LANES)]
        vmem = [((2 * m_in, tokens), jnp.bfloat16), ((2 * m_out, tokens), jnp.bfloat16), ((slots, tokens, STRIPE), jnp.bfloat16),
                ((n_in, m_in, STRIPE), F32), ((n_out, m_out, STRIPE), F32), ((1 + 2 * stripes, 2, LANES), F32),
                ((early // 2, n // 2, 4, 2, LANES), F32), ((single, n // 2, 2, 2, LANES), F32), ((n // 2, 2, LANES), F32), ((n, 2, 2, LANES), F32), ((2, 1 + 2 * stripes, 2, LANES), F32),
                ((kinds, 2 * m_in, LANES), F32), ((2 * m_out, LANES), F32), ((kinds, m_in, LANES), F32), ((m_out, LANES), F32), ((2, 2 * m_in, HALF), F32),
                ((1, LANES), F32), ((n, 1, LANES), F32),
                (row_in.shape, F32), (col_in.shape, F32), ((1, m_out), F32), ((cols_out // LANES, LANES), F32)]
        vmem.append(((8, LANES), F32))
        sems = [(AHEAD,), (2,), (2, 2), (2, 2), (2,), (2,), (2,), (2,), (2,), (2, 2), (2,)]
        anywhere = pl.BlockSpec(memory_space=pl.ANY)
        mid = pl.pallas_call(
            lambda *refs: grads_kernel(n, *refs),
            out_shape=[pltpu.VMEM(s, F32) for s in outs],
            in_specs=[anywhere] * len(ins),
            out_specs=[inside] * len(outs),
            scratch_shapes=[pltpu.VMEM(*v) for v in vmem] + [pltpu.SemaphoreType.DMA(s) for s in sems],
            compiler_params=pltpu.CompilerParams(collective_id=0, has_side_effects=True, vmem_limit_bytes=56 * 2**20),
            name='grads',
        )(*ins)
        finals = [w_in.shape, row_in.shape, col_in.shape, w_out.shape, (1, m_out), (cols_out // LANES, LANES)]
        new = pl.pallas_call(
            apply_kernel,
            out_shape=[jax.ShapeDtypeStruct(s, F32) for s in finals],
            in_specs=[inside] * len(mid),
            out_specs=[anywhere] * len(finals),
            scratch_shapes=[pltpu.VMEM(w_in.shape, F32), pltpu.VMEM(w_out.shape, F32), pltpu.SemaphoreType.DMA((6,))],
            compiler_params=pltpu.CompilerParams(vmem_limit_bytes=8 * 2**20),
            name='apply',
        )(*mid)
        return (new[0], new[1], new[2], new[3], new[4].reshape(m_out), new[5].reshape(cols_out))

    in_specs = (P(None, 'tp'), P(None, 'tp'), P(), P(), P(None, 'tp', None), P('tp', None),
                P(None, 'tp'), P(), P('tp'), P(), P(), P(), P(), P())
    out_specs = (P(None, 'tp', None), P(None, 'tp'), P(), P('tp', None), P('tp'), P())
    return jax.shard_map(local_step, mesh=mesh, in_specs=in_specs, out_specs=out_specs, check_vma=False)
```

```python
import jax
import jax.numpy as jnp
from jax import lax
from jax.experimental import pallas as pl
from jax.experimental.pallas import tpu as pltpu
from jax.sharding import PartitionSpec as P

EPS_ONE = 1e-30
EPS_TWO = 1e-3
LANES = 128
STRIPE = 512
HALF = STRIPE // 2
PARTS = 4
AHEAD = 6
F32 = jnp.float32
MESH = pl.DeviceIdType.MESH


def grads_kernel(n, x_hbm, h_hbm, dyi_hbm, dyo_hbm, wi_hbm, wo_hbm, ri_hbm, ci_hbm, ro_hbm, co_hbm,
                 scal_hbm,
                 gi, go, wi, wo, ri_new, ci_new, ro_new, co_new, coef, ai, ao, colf,
                 xs, hs, dy, si, so, csend, land, mid_land, misc_land, last_land, csum, ri_sq, ro_sq, ri_got, ro_got, split,
                 fsend, f_land, ri, ci, ro, co, scal,
                 dy_sem, xs_sem, g_sem, land_sem, mid_sem, misc_sem, last_sem, fwd_sem, row_sem, f_sem):
    me = lax.axis_index('tp')
    core = lax.rem(me, 2)
    chip = me // 2
    x, y, z = lax.rem(chip, 2), lax.rem(chip // 2, 2), chip // 4
    partner = me + 1 - 2 * core
    high = z // 2
    planes = [3 * (1 - high), 2 - high, z + 1 - 2 * lax.rem(z, 2), z]
    same, everyone = [], []
    for plane in planes:
        for far_y in (1, 0):
            for far_x in (1, 0):
                for other in (0, 1):
                    if plane is z and not (far_y or far_x or other):
                        continue
                    place = (plane * 2 + lax.rem(y + far_y, 2)) * 2 + lax.rem(x + far_x, 2)
                    everyone.append(2 * place + lax.rem(core + other, 2))
                    if not other:
                        same.append(everyone[-1])
    kinds, m_in, cols_in = wi.shape
    m_out, cols_out = wo.shape
    half_in, half_out = cols_in // 2, cols_out // 2
    per_in, per_out = half_in // STRIPE, half_out // STRIPE
    n_in = kinds * per_in
    stripes = n_in + per_out
    slots, tokens = dy.shape[0:2]
    early = 2 * land.shape[0]
    single = mid_land.shape[0]
    shared = early + single

    def remote(src, dst, sems, peer):
        return pltpu.make_async_remote_copy(src_ref=src, dst_ref=dst, send_sem=sems.at[0], recv_sem=sems.at[1],
                                            device_id=(peer,), device_id_type=MESH)

    def to_all(src, dst, sems, who):
        for peer in who:
            remote(src, dst, sems, peer).start()

    def wait_for(ref, sem):
        pltpu.make_async_copy(ref, ref, sem).wait()

    def out_copy(s):
        cols = pl.ds(pl.multiple_of(core * half_out + s * STRIPE, LANES), STRIPE)
        return pltpu.make_async_copy(dyo_hbm.at[:, cols], dy.at[s], dy_sem.at[s + AHEAD // 2])

    def in_copy(t):
        slot = lax.rem(t + per_out, slots)
        cols = pl.ds(pl.multiple_of(core * half_in + lax.rem(t, per_in) * STRIPE, LANES), STRIPE)
        return pltpu.make_async_copy(dyi_hbm.at[t // per_in, :, cols], dy.at[slot], dy_sem.at[lax.rem(t, AHEAD)])

    def last_copy(part):
        t = n_in - 1
        slot = (t + per_out) % slots
        some = pl.ds(part * (tokens // PARTS), tokens // PARTS)
        cols = pl.ds(pl.multiple_of(core * half_in + t % per_in * STRIPE, LANES), STRIPE)
        return pltpu.make_async_copy(dyi_hbm.at[t // per_in, some, cols], dy.at[slot, some, :], dy_sem.at[(t + part) % AHEAD])

    barrier = pltpu.get_barrier_semaphore()
    x_copy = pltpu.make_async_copy(x_hbm, xs.at[pl.ds(0, m_in)], xs_sem.at[0, 0])
    h_copy = pltpu.make_async_copy(h_hbm, hs.at[pl.ds(0, m_out)], xs_sem.at[1, 0])
    x_copy.start()
    h_copy.start()
    out_copy(0).start()
    for peer in everyone:
        pl.semaphore_signal(barrier, inc=1, device_id=(peer,), device_id_type=MESH)
    for s in range(1, per_out):
        out_copy(s).start()
    small = [pltpu.make_async_copy(src, dst, sem.at[0]) for src, dst, sem in (
        (ri_hbm, ri, land_sem), (ci_hbm, ci, mid_sem), (ro_hbm, ro, misc_sem), (co_hbm, co, last_sem), (scal_hbm, scal, fwd_sem))]
    for copy in small:
        copy.start()

    def put_cols(p, h, col_sq, add):
        for r in range(2):
            part = col_sq[:, r * LANES:(r + 1) * LANES]
            where = (1 + 2 * p + h, pl.ds(r, 1), slice(None))
            csend[where] = csend[where] + part if add else part

    def share(pair):
        mine = csend.at[pl.ds(1 + 4 * pair, 4)]
        to_all(mine, land.at[pair, chip], land_sem, same)
        land[pair, chip] = mine[...]

    def add_rows(ref, where, sq):
        ref[where] = ref[where] + (sq[:, 0:LANES] + sq[:, LANES:HALF])

    ri_sq[...] = jnp.zeros_like(ri_sq)
    ro_sq[...] = jnp.zeros_like(ro_sq)
    x_copy.wait()
    h_copy.wait()
    in_copy(0).start()
    in_copy(1).start()
    in_copy(2).start()
    pl.semaphore_wait(barrier, n - 1)
    h_send = remote(hs.at[pl.ds(0, m_out)], hs.at[pl.ds(m_out, m_out)], xs_sem.at[1], partner)
    x_send = remote(xs.at[pl.ds(0, m_in)], xs.at[pl.ds(m_in, m_in)], xs_sem.at[0], partner)
    x_send.start()
    h_send.start()

    for s in range(per_out):
        out_copy(s).wait()
        in_copy(s + 3).start()
        for h in range(2):
            cols = pl.ds(h * HALF, HALF)
            own = jnp.dot(hs[0:m_out, :], dy[s, :, cols], preferred_element_type=F32)
            go[s, core, :, cols] = own
            own = own * own
            put_cols(s, h, jnp.sum(own, axis=0, keepdims=True), False)
            add_rows(ro_sq, (pl.ds(0, m_out), slice(None)), own)
    for copy in small:
        copy.wait()
    lane = lax.broadcasted_iota(jnp.int32, (1, LANES), 1)

    def pack(values):
        row = jnp.zeros((1, LANES), F32)
        for i, value in enumerate(values):
            row = jnp.where(lane == i, value, row)
        return row

    csend[0, 1:2, :] = jnp.zeros((1, LANES), F32)
    csend[0, 0:1, :] = pack([jnp.sum(ri[k:k + 1, :], axis=1, keepdims=True) for k in range(kinds)]
                            + [jnp.sum(ro[...], axis=1, keepdims=True)]) + scal[0:1, :]
    to_all(csend.at[0], misc_land.at[chip], misc_sem, same)
    misc_land[chip] = csend[0]
    x_send.wait_recv()
    in_copy(5).start()

    def partner_rows():
        h_send.wait_recv()
        for s in range(per_out):
            for h in range(2):
                cols = pl.ds(h * HALF, HALF)
                other = jnp.dot(hs[m_out:2 * m_out, :], dy[s, :, cols], preferred_element_type=F32)
                so[s, :, cols] = other
                other = other * other
                put_cols(s, h, jnp.sum(other, axis=0, keepdims=True), True)
                add_rows(ro_sq, (pl.ds(m_out, m_out), slice(None)), other)
        remote(so, go.at[:, core], g_sem.at[0], partner).start()
        remote(ro_sq.at[pl.ds(m_out, m_out)], ro_got, row_sem.at[0], partner).start()
        share(0)

    def product(t):
        p = t + per_out
        for h in range(2):
            cols = pl.ds(h * HALF, HALF)
            both = jnp.dot(xs[...], dy[lax.rem(p, slots), :, cols], preferred_element_type=F32)
            gi[t, core, :, cols] = both[0:m_in]
            si[t, :, cols] = both[m_in:2 * m_in]
            both = both * both
            put_cols(p, h, jnp.sum(both, axis=0, keepdims=True), False)
            add_rows(ri_sq, t // per_in, both)

    def give(t, size):
        remote(si.at[pl.ds(t, size)], gi.at[pl.ds(t, size), core], g_sem.at[1], partner).start()

    def in_step(i, carry):
        @pl.when(i == 1)
        def _():
            partner_rows()

        for t in (2 * i, 2 * i + 1):
            in_copy(t).wait()

            @pl.when(t + AHEAD < n_in - 1)
            def _():
                in_copy(t + AHEAD).start()

            for part in range(PARTS):
                @pl.when(t + AHEAD == n_in - 1 + part)
                def _():
                    last_copy(part).start()

        for t in (2 * i, 2 * i + 1):
            product(t)
        share(i + 1)
        give(2 * i, 2)
        return carry

    lax.fori_loop(0, early // 2 - 1, in_step, 0)
    def single_step(t, carry):
        in_copy(t).wait()
        for part in range(PARTS):
            @pl.when(t + AHEAD == n_in - 1 + part)
            def _():
                last_copy(part).start()

        product(t)
        p = t + per_out
        mine = csend.at[pl.ds(1 + 2 * p, 2)]
        to_all(mine, mid_land.at[p - early, chip], mid_sem, same)
        mid_land[p - early, chip] = mine[...]
        give(t, 1)
        return carry

    lax.fori_loop(early - per_out, n_in - 1, single_step, 0)
    t = n_in - 1
    for part in range(PARTS):
        some = pl.ds(part * (tokens // PARTS), tokens // PARTS)
        last_copy(part).wait()
        if part == PARTS - 1:
            x_send.wait_send()
            h_send.wait_send()
            wi_copy = pltpu.make_async_copy(wi_hbm, wi, xs_sem.at[0, 0])
            wo_copy = pltpu.make_async_copy(wo_hbm, wo, xs_sem.at[1, 0])
            wi_copy.start()
            wo_copy.start()
        for h in range(2):
            cols = pl.ds(h * HALF, HALF)
            both = jnp.dot(xs[:, some], dy[(t + per_out) % slots, some, cols], preferred_element_type=F32)
            if part:
                both = split[h] + both
            if part < PARTS - 1:
                split[h] = both
                continue
            gi[t, core, :, cols] = both[0:m_in]
            si[t, :, cols] = both[m_in:2 * m_in]
            both = both * both
            put_cols(t + per_out, h, jnp.sum(both, axis=0, keepdims=True), False)
            add_rows(ri_sq, t // per_in, both)
    mine = csend.at[pl.ds(1 + 2 * shared, 2)]
    to_all(mine, last_land.at[me], last_sem, everyone)
    last_land[me] = mine[...]
    remote(ri_sq.at[:, pl.ds(m_in, m_in)], ri_got, row_sem.at[1], partner).start()
    give(n_in - 1, 1)
    wait_for(misc_land.at[pl.ds(0, n // 2 - 1)], misc_sem.at[1])
    wait_for(land.at[:, pl.ds(0, n // 2 - 1)], land_sem.at[1])
    csum[core, 0] = jnp.sum(misc_land[...], axis=0)
    for pair in range(early // 2):
        csum[core, pl.ds(1 + 4 * pair, 4)] = jnp.sum(land[pair], axis=0)
    wait_for(mid_land.at[:, pl.ds(0, n // 2 - 1)], mid_sem.at[1])
    for i in range(single):
        csum[core, pl.ds(1 + 2 * (early + i), 2)] = jnp.sum(mid_land[i], axis=0)
    done = csum.at[core, pl.ds(0, 1 + 2 * shared)]
    forward = remote(done, done, fwd_sem, partner)
    forward.start()
    wait_for(ro_got, row_sem.at[0, 1])
    wait_for(ri_got, row_sem.at[1, 1])
    row_sums = [jnp.sum(ri_sq[k, 0:m_in] + ri_got[k], axis=1, keepdims=True) for k in range(kinds)]
    row_sums.append(jnp.sum(ro_sq[0:m_out] + ro_got[...], axis=1, keepdims=True))
    def square_sum(ref, cols):
        rows = ref.shape[0]
        total = [jnp.zeros((8, LANES), F32) for _ in range(4)]
        for r in range(cols // LANES):
            for b in range(rows // 8):
                w = ref[8 * b:8 * (b + 1), r * LANES:(r + 1) * LANES]
                total[b % 4] = total[b % 4] + w * w
        total = (total[0] + total[1]) + (total[2] + total[3])
        return jnp.sum(jnp.sum(total, axis=0, keepdims=True), axis=1, keepdims=True)

    wi_copy.wait()
    wo_copy.wait()
    w_sums = [square_sum(wi.at[k], cols_in) for k in range(kinds)] + [square_sum(wo, cols_out)]
    forward.wait_recv()
    first = [1 + 2 * (per_out + k * per_in) for k in range(kinds)] + [1]
    count = [2 * per_in] * kinds + [2 * per_out]
    rows_of = [m_in * n] * kinds + [m_out * n]
    cols_of = [cols_in] * kinds + [cols_out]

    def at_lane(row, i):
        return jnp.sum(jnp.where(lane == i, row, 0.0), axis=1, keepdims=True)

    misc = csum[0, 0, 0:1, :] + csum[1, 0, 0:1, :]
    keep, norm, step, rms = (at_lane(misc, kinds + 1 + i) for i in range(4))
    mix = 1.0 - keep
    eyes, olds, levels, grand = [], [], [], []
    for i in range(kinds + 1):
        rows = m_out if i == kinds else m_in
        eyes.append(lax.broadcasted_iota(jnp.int32, (rows, rows), 0) == lax.broadcasted_iota(jnp.int32, (rows, rows), 1))
        old = ro[...] if i == kinds else ri[i:i + 1, :]
        olds.append(keep * jnp.sum(jnp.where(eyes[i], old, 0.0), axis=1, keepdims=True))
        levels.append(keep * (at_lane(misc, i) / rows_of[i]))
        known = min(first[i] + count[i], 1 + 2 * shared)
        grand.append(jnp.sum(csum[:, first[i]:known], axis=(0, 1)))
    wait_for(last_land.at[pl.ds(0, n - 1)], last_sem.at[1])
    for c in range(2):
        total = last_land[c]
        for q in range(1, n // 2):
            total = total + last_land[2 * q + c]
        csum[c, pl.ds(1 + 2 * shared, 2)] = total
        grand[kinds - 1] = grand[kinds - 1] + jnp.sum(total, axis=0)
    grand = [jnp.sum(jnp.sum(g, axis=0, keepdims=True), axis=1, keepdims=True) for g in grand]
    norm_sq = grand[0]
    for g in grand[1:]:
        norm_sq = norm_sq + g
    scale = jnp.minimum(1.0, norm / jnp.sqrt(norm_sq))

    for i in range(kinds + 1):
        rows = m_out if i == kinds else m_in
        level = levels[i] + mix * (scale * (scale * (grand[i] / (rows_of[i] * cols_of[i]))) + EPS_ONE)
        new = olds[i] + mix * (scale * (scale * (row_sums[i] / cols_of[i])) + EPS_ONE)
        factor = jnp.broadcast_to(scale * lax.rsqrt(new / level), (rows, LANES))
        if i == kinds:
            ao[...] = factor
        else:
            ai[i] = factor
        olds[i] = new

    for c in range(2):
        for p in range(stripes):
            for r in range(STRIPE // LANES):
                where = (c, 1 + 2 * p + r // 2, pl.ds(r % 2, 1), slice(None))
                if p < per_out:
                    i = kinds
                    spot = (pl.ds((c * half_out + p * STRIPE) // LANES + r, 1), slice(None))
                    old, store = co, co_new
                else:
                    i, s = divmod(p - per_out, per_in)
                    spot = (pl.ds(i, 1), pl.ds(c * half_in + s * STRIPE + r * LANES, LANES))
                    old, store = ci, ci_new
                new = keep * old[spot] + mix * (scale * (scale * (csum[where] / rows_of[i])) + EPS_ONE)
                store[spot] = new
                colf[c, STRIPE // LANES * p + r] = lax.rsqrt(new)

    wait_for(so, g_sem.at[0, 1])
    wait_for(si, g_sem.at[1, 1])
    def update_sq(ref, factor, p0, blocks):
        rows = ref.shape[2]
        spots = [(t, c, r) for t in range(*blocks) for c in range(2) for r in range(STRIPE // LANES)]
        totals = [None] * len(spots)
        for b in range(rows // 8):
            some = slice(8 * b, 8 * (b + 1))
            weight = factor[some, :]
            for i, (t, c, r) in enumerate(spots):
                part = ref[t, c, some, r * LANES:(r + 1) * LANES] * weight
                part = part * part
                totals[i] = part if totals[i] is None else totals[i] + part
        parts = []
        for (t, c, r), total in zip(spots, totals):
            col = colf[c, STRIPE // LANES * (p0 + t) + r]
            parts.append(total * (col * col))
        while len(parts) > 1:
            parts = [a + b for a, b in zip(parts[::2], parts[1::2])] + parts[len(parts) // 2 * 2:]
        return jnp.sum(jnp.sum(parts[0], axis=0, keepdims=True), axis=1, keepdims=True)

    u_sums = [update_sq(gi, ai.at[k], per_out, (k * per_in, (k + 1) * per_in)) for k in range(kinds)]
    u_sums.append(update_sq(go, ao, 0, (0, per_out)))
    fsend[...] = pack(u_sums + w_sums)
    to_all(fsend, f_land.at[me], f_sem, everyone)
    f_land[me] = fsend[...]

    for i in range(kinds + 1):
        flat = jnp.sum(jnp.where(eyes[i], olds[i], 0.0), axis=0, keepdims=True)
        if i == kinds:
            ro_new[...] = flat
        else:
            ri_new[i:i + 1, :] = flat

    forward.wait_send()
    wait_for(so, g_sem.at[0, 0])
    wait_for(si, g_sem.at[1, 0])
    wait_for(misc_land.at[pl.ds(0, n // 2 - 1)], misc_sem.at[0])
    wait_for(land.at[:, pl.ds(0, n // 2 - 1)], land_sem.at[0])
    wait_for(mid_land.at[:, pl.ds(0, n // 2 - 1)], mid_sem.at[0])
    wait_for(ro_got, row_sem.at[0, 0])
    wait_for(ri_got, row_sem.at[1, 0])
    wait_for(last_land.at[pl.ds(0, n - 1)], last_sem.at[0])
    wait_for(f_land.at[pl.ds(0, n - 1)], f_sem.at[1])
    parts = [f_land[d] for d in range(n)]
    while len(parts) > 1:
        parts = [a + b for a, b in zip(parts[::2], parts[1::2])]
    sums = parts[0]
    for i in range(kinds + 1):
        size = float(rows_of[i] * cols_of[i])
        clip = jnp.maximum(1.0, jnp.sqrt(at_lane(sums, i) / size) / rms)
        move = step * jnp.maximum(EPS_TWO, jnp.sqrt(at_lane(sums, kinds + 1 + i) / size))
        coef[i:i + 1, :] = jnp.broadcast_to(move / clip, (1, LANES))
    wait_for(f_land.at[pl.ds(0, n - 1)], f_sem.at[0])


def scalar_kernel(place, one, two, row):
    lane = lax.broadcasted_iota(jnp.int32, (8, LANES), 1)
    row[...] = jnp.where(lane == place, one[...], jnp.where(lane == place + 1, two[...], 0.0))


def apply_kernel(gi, go, wi, wo, ri, ci, ro, co, coef, ai, ao, colf, wi_out, ri_out, ci_out, wo_out, ro_out, co_out, wi_new, wo_new, sems):
    kinds, m_in, cols_in = wi.shape
    per_in, per_out = gi.shape[0] // kinds, go.shape[0]
    lanes = STRIPE // LANES

    def send(src, dst, sem):
        copy = pltpu.make_async_copy(src, dst, sems.at[sem])
        copy.start()
        return copy

    def blocks(factor, g, p, c, old, new, out, first, sem):
        for r in range(lanes):
            cols = pl.ds(first + r * LANES, LANES)
            new[:, cols] = old[:, cols] - (factor * colf[c, lanes * p + r]) * g[:, r * LANES:(r + 1) * LANES]
        part = pl.ds(first, STRIPE)
        send(new.at[:, part], out.at[:, part], sem)

    small = [send(src, dst, 2 + i) for i, (src, dst) in enumerate(((ri, ri_out), (ci, ci_out), (ro, ro_out), (co, co_out)))]
    for c in range(2):
        factor = ao[...] * coef[kinds:kinds + 1, :]
        for s in range(per_out):
            blocks(factor, go.at[s, c], s, c, wo, wo_new, wo_out, c * (wo.shape[1] // 2) + s * STRIPE, 0)
    for k in range(kinds):
        factor = ai[k] * coef[k:k + 1, :]
        for c in range(2):
            for s in range(per_in):
                t = k * per_in + s
                blocks(factor, gi.at[t, c], per_out + t, c, wi.at[k], wi_new.at[k], wi_out.at[k], c * (cols_in // 2) + s * STRIPE, 1)
    for copy in small:
        copy.wait()
    pltpu.make_async_copy(wo_new, wo_out, sems.at[0]).wait()
    pltpu.make_async_copy(wi_new, wi_out, sems.at[1]).wait()


def solution(mesh):
    n = mesh.shape['tp']

    def local_step(x_norm, hid_act, dy_in, dy_out, w_in, w_out, row_in, col_in, row_out, col_out, beta_two, rel_step, clip_rms, clip_norm):
        kinds, m_in, cols_in = w_in.shape
        m_out, cols_out = w_out.shape
        tokens = x_norm.shape[0]
        inside = pl.BlockSpec(memory_space=pltpu.VMEM)
        scalars = lax.switch(
            jnp.minimum(lax.axis_index('tp'), 2),
            [lambda *values, i=i: pl.pallas_call(
                lambda *refs: scalar_kernel(kinds + 1 + 2 * i, *refs), out_shape=jax.ShapeDtypeStruct((8, LANES), F32),
                in_specs=[inside] * 2, out_specs=inside, name='scalar')(*[v.reshape(1, 1) for v in values[2 * i:2 * i + 2]]) for i in range(2)]
            + [lambda *values: jnp.zeros((8, LANES), F32)],
            beta_two, clip_norm, rel_step, clip_rms)
        n_in, n_out = kinds * cols_in // (2 * STRIPE), cols_out // (2 * STRIPE)
        stripes = n_in + n_out
        single = 3
        early = stripes - single - 1
        slots = 10
        ins = [x_norm.T, hid_act.T, dy_in, dy_out, w_in, w_out, row_in, col_in, row_out.reshape(1, -1), col_out.reshape(-1, LANES)]
        ins.append(scalars)
        outs = [(n_in, 2, m_in, STRIPE), (n_out, 2, m_out, STRIPE), w_in.shape, w_out.shape, row_in.shape, col_in.shape,
                (1, m_out), (cols_out // LANES, LANES), (8, LANES), (kinds, m_in, LANES), (m_out, LANES), (2, stripes * STRIPE // LANES, 1, LANES)]
        vmem = [((2 * m_in, tokens), jnp.bfloat16), ((2 * m_out, tokens), jnp.bfloat16), ((slots, tokens, STRIPE), jnp.bfloat16),
                ((n_in, m_in, STRIPE), F32), ((n_out, m_out, STRIPE), F32), ((1 + 2 * stripes, 2, LANES), F32),
                ((early // 2, n // 2, 4, 2, LANES), F32), ((single, n // 2, 2, 2, LANES), F32), ((n // 2, 2, LANES), F32), ((n, 2, 2, LANES), F32), ((2, 1 + 2 * stripes, 2, LANES), F32),
                ((kinds, 2 * m_in, LANES), F32), ((2 * m_out, LANES), F32), ((kinds, m_in, LANES), F32), ((m_out, LANES), F32), ((2, 2 * m_in, HALF), F32),
                ((1, LANES), F32), ((n, 1, LANES), F32),
                (row_in.shape, F32), (col_in.shape, F32), ((1, m_out), F32), ((cols_out // LANES, LANES), F32)]
        vmem.append(((8, LANES), F32))
        sems = [(AHEAD,), (2, 2), (2, 2), (2,), (2,), (2,), (2,), (2,), (2, 2), (2,)]
        anywhere = pl.BlockSpec(memory_space=pl.ANY)
        mid = pl.pallas_call(
            lambda *refs: grads_kernel(n, *refs),
            out_shape=[pltpu.VMEM(s, F32) for s in outs],
            in_specs=[anywhere] * len(ins),
            out_specs=[inside] * len(outs),
            scratch_shapes=[pltpu.VMEM(*v) for v in vmem] + [pltpu.SemaphoreType.DMA(s) for s in sems],
            compiler_params=pltpu.CompilerParams(collective_id=0, has_side_effects=True, vmem_limit_bytes=56 * 2**20),
            name='grads',
        )(*ins)
        finals = [w_in.shape, row_in.shape, col_in.shape, w_out.shape, (1, m_out), (cols_out // LANES, LANES)]
        new = pl.pallas_call(
            apply_kernel,
            out_shape=[jax.ShapeDtypeStruct(s, F32) for s in finals],
            in_specs=[inside] * len(mid),
            out_specs=[anywhere] * len(finals),
            scratch_shapes=[pltpu.VMEM(w_in.shape, F32), pltpu.VMEM(w_out.shape, F32), pltpu.SemaphoreType.DMA((6,))],
            compiler_params=pltpu.CompilerParams(vmem_limit_bytes=8 * 2**20),
            name='apply',
        )(*mid)
        return (new[0], new[1], new[2], new[3], new[4].reshape(m_out), new[5].reshape(cols_out))

    in_specs = (P(None, 'tp'), P(None, 'tp'), P(), P(), P(None, 'tp', None), P('tp', None),
                P(None, 'tp'), P(), P('tp'), P(), P(), P(), P(), P())
    out_specs = (P(None, 'tp', None), P(None, 'tp'), P(), P('tp', None), P('tp'), P())
    return jax.shard_map(local_step, mesh=mesh, in_specs=in_specs, out_specs=out_specs, check_vma=False)
```
